32 devices in a mesh: sp: 16 (over z, y, core), dp: 2 (over x).
Axes of the slice: x: 2, y: 2, z: 4, core: 2. Of those that a mesh axis runs over, the one named last changes fastest.
Arguments:
- query_proj: bfloat16 [4096, 8192], P(('dp', 'sp')), parts along dimension 0, may hold values from -64 to 64
- key_projection: bfloat16 [4096, 1024], P(('dp', 'sp')), parts along dimension 0, may hold values from -64 to 64
- value_projection: bfloat16 [4096, 1024], P(('dp', 'sp')), parts along dimension 0, may hold values from -12 to 12
- query_gain: float32 [128], replicated, may hold values from 1 to 5
- key_norm_gain: float32 [128], replicated, may hold values from 1 to 5
- positions: int32 [4096], P(('dp', 'sp')), parts along dimension 0, may hold values from 0 to 5118, as said below
- doc_start: int32 [4096], P(('dp', 'sp')), parts along dimension 0, may hold values from 0 to 2047, as said below
Outputs:
- attention: bfloat16 [4096, 8192], P(('dp', 'sp')), parts along dimension 0
The draws below stay inside these ranges and needn't reach their ends.
There are 2 independent parts, one for each index of `dp`. The reference program is written for one: setup_inputs(seed, part) draws one part's arguments, and reference() takes and returns one part's arrays. A program takes and returns all parts, laid end to end along the dimension named above; an argument that names none is the same for every part. Nothing has to cross between parts.
Inputs may be any that keep to these rules, and one draw needn't show every extreme that they name: doc_start[i] is the index of the first token of token i's document: it never falls, doc_start[i] <= i < doc_start[i] + 1024, some document has exactly 1024 tokens, and every document but the last has 128 tokens or more. `positions`: within one document the position rises by one from each token to the next.
All inputs are finite; a program needn't handle non-finite values.
Results may differ from the reference program's by a relative error of at most 0.0039.
The reference program's roundings to bfloat16 on the way count: a program that leaves them out, or rounds other values in their place, can miss the bound.
Values may be sent and summed in bfloat16 or wider, within the bound.
A program may use at most 64 MiB of HBM per device.

```python
import jax
import jax.numpy as jnp
from jax import lax

QUERY_HEADS = 64
KEY_VALUE_HEADS = 8
HEAD_SIZE = 128
DOC_MAX = 1024
PACK_TOKENS = 2048


def doc_layout(key):
    rotary_base = jax.random.fold_in(key, 11)
    shortest = DOC_MAX // 8
    count = PACK_TOKENS // shortest + 1
    lengths = jax.random.randint(jax.random.fold_in(rotary_base, 1), (count,), shortest, DOC_MAX + 1, dtype=jnp.int32)
    forced = jax.random.randint(jax.random.fold_in(rotary_base, 2), (), 0, 2, dtype=jnp.int32)
    lengths = jnp.where(jnp.arange(count, dtype=jnp.int32) == forced, DOC_MAX, lengths).astype(jnp.int32)
    starts = (jnp.cumsum(lengths) - lengths).astype(jnp.int32)
    token_index = jnp.arange(PACK_TOKENS, dtype=jnp.int32)
    doc_index = jnp.sum((starts[None, :] <= token_index[:, None]).astype(jnp.int32), axis=1) - 1
    doc_first = starts[doc_index]
    offsets = jax.random.randint(jax.random.fold_in(rotary_base, 3), (count,), 0, 4 * DOC_MAX, dtype=jnp.int32)
    positions = offsets[doc_index] + token_index - doc_first
    return (doc_first.astype(jnp.int32), positions.astype(jnp.int32))


def qk_fields(key):
    rotary_base = jax.random.fold_in(key, 23)
    q_vals = jax.random.normal(jax.random.fold_in(rotary_base, 1), (PACK_TOKENS, QUERY_HEADS, HEAD_SIZE), jnp.float32)
    key_values_local = jax.random.normal(jax.random.fold_in(rotary_base, 2), (PACK_TOKENS, KEY_VALUE_HEADS, HEAD_SIZE), jnp.float32)
    q_vals = jnp.clip(q_vals, -64.0, 64.0).reshape(PACK_TOKENS, QUERY_HEADS * HEAD_SIZE)
    key_values_local = jnp.clip(key_values_local, -64.0, 64.0).reshape(PACK_TOKENS, KEY_VALUE_HEADS * HEAD_SIZE)
    return (q_vals, key_values_local)


def draw_query_proj(key, part):
    return qk_fields(key)[0].astype(jnp.bfloat16)


def draw_key_projection(key, part):
    return qk_fields(key)[1].astype(jnp.bfloat16)


def draw_query_gain(key, part):
    sub_key = jax.random.fold_in(key, 31)
    return jax.random.uniform(sub_key, (HEAD_SIZE,), jnp.float32, 1.0, 2.0)


def draw_key_norm_gain(key, part):
    sub_key = jax.random.fold_in(key, 37)
    return jax.random.uniform(sub_key, (HEAD_SIZE,), jnp.float32, 1.0, 2.0)


def draw_positions(key, part):
    return doc_layout(key)[1]


def draw_doc_start(key, part):
    return doc_layout(key)[0]


def block_levels(rng, dims, pieces, smallest, largest):
    loudness, own = 1.0, jax.random.fold_in(rng, 6)
    for axis_at, blocks in pieces:
        steps = jnp.exp(jax.random.uniform(jax.random.fold_in(own, axis_at), (blocks,), jnp.float32, smallest / len(pieces), largest / len(pieces)))
        loudness = loudness * jnp.repeat(steps, dims[axis_at] // blocks).reshape([-1 if axis == axis_at else 1 for axis in range(len(dims))])
    return loudness


def normal_values(own_key, extent, spread, reach, split=(), held_as=jnp.bfloat16):
    drawn = spread * jax.random.normal(own_key, extent, jnp.float32)
    if split:
        drawn = drawn * block_levels(own_key, extent, split, -0.22, 0.18)
    return jnp.clip(drawn, -reach, reach).astype(held_as)


def setup_inputs(seed: int = 0, part: int = 0) -> dict:
    key_of = jax.random.split(jax.random.key(seed), 8)
    own_keys = jax.random.split(jax.random.fold_in(key_of[7], part), 8)
    return {
        "query_proj": draw_query_proj(jax.random.fold_in(jax.random.fold_in(key_of[7], part), 71), part),
        "key_projection": draw_key_projection(jax.random.fold_in(jax.random.fold_in(key_of[7], part), 71), part),
        "value_projection": normal_values(own_keys[2], (PACK_TOKENS, KEY_VALUE_HEADS * HEAD_SIZE), 2.0, 12.0, ((0, 16),)),
        "query_gain": draw_query_gain(jax.random.fold_in(key_of[7], 71), part),
        "key_norm_gain": draw_key_norm_gain(jax.random.fold_in(key_of[7], 71), part),
        "positions": draw_positions(jax.random.fold_in(jax.random.fold_in(key_of[7], part), 71), part),
        "doc_start": draw_doc_start(jax.random.fold_in(jax.random.fold_in(key_of[7], part), 71), part),
    }


ROPE_BASE = 1000000.0
NORM_EPS = 1e-06

def rotary_tables(positions):
    half_dim = HEAD_SIZE // 2
    inv_freq = ROPE_BASE ** (-(jnp.arange(half_dim, dtype=jnp.float32) * 2.0 / HEAD_SIZE))
    angle = positions.astype(jnp.float32)[:, None] * inv_freq[None, :]
    return (jnp.cos(angle), jnp.sin(angle))

def normalize_and_rotate(heads_in, gain, cosine_table, sine_table):
    upcast = heads_in.astype(jnp.float32)
    mean_square = lax.optimization_barrier(jnp.mean(upcast * upcast, axis=-1, keepdims=True))
    normed = upcast * lax.rsqrt(mean_square + NORM_EPS) * gain
    half_dim = normed.shape[-1] // 2
    first_half = normed[..., :half_dim]
    second_half = normed[..., half_dim:]
    cos_rows = cosine_table[:, None, :]
    sin_rows = sine_table[:, None, :]
    rotated = jnp.concatenate([first_half * cos_rows - second_half * sin_rows, second_half * cos_rows + first_half * sin_rows], axis=-1)
    return rotated.astype(jnp.bfloat16)

def attend(q_head, k_head, v_head, starts):
    rows_all = q_head.shape[0]
    block_rows = min(512, rows_all)
    key_window = DOC_MAX + block_rows
    zero_rows = jnp.zeros((DOC_MAX, q_head.shape[1]), q_head.dtype)
    k_padded = jnp.concatenate([zero_rows, k_head], axis=0)
    v_padded = jnp.concatenate([zero_rows, v_head], axis=0)
    scale = q_head.shape[1] ** (-0.5)

    def one_block(block_index):
        block_start = (block_index * block_rows).astype(jnp.int32)
        query_block = lax.dynamic_slice_in_dim(q_head, block_start, block_rows, 0)
        key_block = lax.dynamic_slice_in_dim(k_padded, block_start, key_window, 0)
        value_block = lax.dynamic_slice_in_dim(v_padded, block_start, key_window, 0)
        doc_first = lax.dynamic_slice_in_dim(starts, block_start, block_rows, 0)
        row_index = block_start + jnp.arange(block_rows, dtype=jnp.int32)
        key_index = block_start - DOC_MAX + jnp.arange(key_window, dtype=jnp.int32)
        visible = (key_index[None, :] >= doc_first[:, None]) & (key_index[None, :] <= row_index[:, None])
        scores = jnp.dot(query_block, key_block.T, preferred_element_type=jnp.float32) * scale
        scores = jnp.where(visible, scores, -jnp.inf)
        row_max = lax.optimization_barrier(jnp.max(scores, axis=1, keepdims=True))
        exp_scores = jnp.exp(scores - row_max)
        row_total = lax.optimization_barrier(jnp.sum(exp_scores, axis=1, keepdims=True))
        weights = exp_scores.astype(jnp.bfloat16)
        mixed_out = jnp.dot(weights, value_block, preferred_element_type=jnp.float32) / row_total
        return mixed_out.astype(jnp.bfloat16)
    blocks = lax.map(one_block, jnp.arange(rows_all // block_rows, dtype=jnp.int32))
    return blocks.reshape(rows_all, q_head.shape[1])

def reference(query_proj, key_projection, value_projection, query_gain, key_norm_gain, positions, doc_start):
    cosine_table, sine_table = rotary_tables(positions)
    q_rope = normalize_and_rotate(query_proj.reshape(PACK_TOKENS, QUERY_HEADS, HEAD_SIZE), query_gain, cosine_table, sine_table)
    key_rotated = normalize_and_rotate(key_projection.reshape(PACK_TOKENS, KEY_VALUE_HEADS, HEAD_SIZE), key_norm_gain, cosine_table, sine_table)
    value_head_split = value_projection.reshape(PACK_TOKENS, KEY_VALUE_HEADS, HEAD_SIZE)
    head_copies = QUERY_HEADS // KEY_VALUE_HEADS
    q_major = jnp.transpose(q_rope, (1, 0, 2))
    k_major = jnp.repeat(jnp.transpose(key_rotated, (1, 0, 2)), head_copies, axis=0)
    v_major = jnp.repeat(jnp.transpose(value_head_split, (1, 0, 2)), head_copies, axis=0)

    def one_head(operands):
        return attend(operands[0], operands[1], operands[2], doc_start)
    per_head = lax.map(one_head, (q_major, k_major, v_major))
    return jnp.transpose(per_head, (1, 0, 2)).reshape(PACK_TOKENS, QUERY_HEADS * HEAD_SIZE)
```

```python
import functools
import math

import jax
import jax.numpy as jnp
import numpy as np
from jax import lax
from jax.experimental import pallas as pl
from jax.experimental.pallas import tpu as pltpu
from jax.sharding import PartitionSpec as P

HEAD_SIZE = 128
DOC_MAX = 1024
REACH = 8
ROPE_BASE = 1000000.0
NORM_EPS = 1e-06
HIDDEN = -1e30
Q_TILE = 2
LEAD = 5
MESH = pl.DeviceIdType.MESH

KEY, VALUE = 0, 1
OWN_Z, OWN_Y, OWN_C, F4_Z, F4_Y, F4_C, F8_Y, F8_C, F2_C, F6_C = range(10)


def norm_rope(block, swap, straight, crossed):
    up = block.astype(jnp.float32)
    mean_square = jnp.mean(up * up, axis=-1, keepdims=True)
    swapped = jnp.dot(block, swap, preferred_element_type=jnp.float32)
    return (up * straight + swapped * crossed) * lax.rsqrt(mean_square + NORM_EPS)


def chunk_order(groups):
    head = min(2, groups)
    order = [(VALUE, g) for g in range(head)] + [(KEY, g) for g in range(head)]
    for g in range(head, groups):
        order += [(KEY, g), (VALUE, g)]
    return order


def kernel(
    count, groups, copies, rows,
    q_hbm, k_hbm, v_hbm, qg_hbm, kg_hbm, freq_hbm, pos_hbm, start_hbm,
    o_hbm, win_k, win_v, hidden, q_ref, k_ref, q_rope, o_ref,
    scores_a, scores_b, top_a, top_b, weights_0, weights_1, weights_2, weights_3,
    qg_ref, kg_ref, freq_ref, pos_ref, start_ref,
    value_sem, in_sem, query_sem, out_sem, send_sem, recv_sem,
):
    me = lax.axis_index("sp")
    core = lax.rem(me, 2)
    side = lax.rem(lax.div(me, 2), 2)
    core_peer = me + 1 - 2 * core
    side_peer = me + 2 - 4 * side
    blocks = REACH + 1
    scores_buf = [scores_a, scores_b]
    top_buf = [top_a, top_b]
    weights_buf = [weights_0, weights_1, weights_2, weights_3]
    tiles = copies // Q_TILE
    tile_rows = Q_TILE * rows

    def chunk(c, g, slot):
        return (win_k, win_v)[c].at[g, REACH - slot]

    def send(kind, c, g, source, target_slot, target):
        return pltpu.make_async_remote_copy(
            src_ref=chunk(c, g, source),
            dst_ref=chunk(c, g, target_slot),
            send_sem=send_sem.at[c, kind],
            recv_sem=recv_sem.at[c, target_slot, g],
            device_id={"sp": target},
            device_id_type=MESH,
        )

    has_next = me + 4 < count
    f4_slot = 6 - 4 * side

    plan = {
        OWN_Z: (has_next, 0, 4, me + 4),
        OWN_Y: (side == 0, 0, 2, side_peer),
        OWN_C: (core == 0, 0, 1, core_peer),
        F4_Z: ((me >= 4) & has_next, 4, 8, me + 4),
        F4_Y: (me >= 4, 4, f4_slot, side_peer),
        F4_C: (me >= 4, 4, 5 - 2 * core, core_peer),
        F8_Y: ((me >= 8) & (side == 1), 8, 6, side_peer),
        F8_C: ((me >= 8) & (core == 1), 8, 7, core_peer),
        F2_C: (me >= 2, 2, 3 - 2 * core, core_peer),
        F6_C: (me >= 6, 6, 7 - 2 * core, core_peer),
    }

    def start(kind, c, g):
        condition, source, target_slot, target = plan[kind]

        @pl.when(condition)
        def _():
            send(kind, c, g, source, target_slot, target).start()

    def arrived(slot, c, g):
        @pl.when(me >= slot)
        def _():
            send(OWN_Z, c, g, 0, slot, me).wait_recv()

    def own(c, g):
        for kind in (OWN_Z, OWN_Y, OWN_C):
            start(kind, c, g)

    forwards = {4: (F4_Z, F4_Y, F4_C), 8: (F8_Y, F8_C), 2: (F2_C,), 6: (F6_C,)}

    def relay(slot, c, g):
        arrived(slot, c, g)
        for kind in forwards[slot]:
            start(kind, c, g)

    value_copies = [
        pltpu.make_async_copy(
            v_hbm.at[:, pl.ds(g * HEAD_SIZE, HEAD_SIZE)],
            win_v.at[g, REACH],
            value_sem.at[g],
        )
        for g in range(groups)
    ]
    small = [
        pltpu.make_async_copy(source, target, in_sem.at[i])
        for i, (source, target) in enumerate([
            (pos_hbm, pos_ref), (freq_hbm, freq_ref), (kg_hbm, kg_ref), (k_hbm, k_ref),
            (start_hbm, start_ref), (qg_hbm, qg_ref),
        ])
    ]
    width = copies * HEAD_SIZE
    query_copies = [
        pltpu.make_async_copy(
            q_hbm.at[:, pl.ds(i * HEAD_SIZE, HEAD_SIZE)], q_ref.at[i], query_sem.at[i // copies]
        )
        for i in range(groups * copies)
    ]
    barrier = pltpu.get_barrier_semaphore()
    for peer in (core_peer, side_peer):
        pl.semaphore_signal(barrier, inc=1, device_id={"sp": peer}, device_id_type=MESH)

    @pl.when(has_next)
    def _():
        pl.semaphore_signal(barrier, inc=1, device_id={"sp": me + 4}, device_id_type=MESH)

    @pl.when(me >= 4)
    def _():
        pl.semaphore_signal(barrier, inc=1, device_id={"sp": me - 4}, device_id_type=MESH)

    for copy in value_copies[:2] + small + value_copies[2:] + query_copies:
        copy.start()

    order = chunk_order(groups)
    head = min(2, groups)
    for copy in value_copies[:head]:
        copy.wait()
    inner = (me >= 4) & has_next

    @pl.when(inner)
    def _():
        pl.semaphore_wait(barrier, 4)

    @pl.when(jnp.logical_not(inner))
    def _():
        pl.semaphore_wait(barrier, 3 if count > 4 else 2)

    for n in range(head):
        own(*order[n])

    for copy in small:
        copy.wait()
    places = jnp.broadcast_to(pos_ref[...].astype(jnp.float32), (HEAD_SIZE, rows)).T
    angle = places * freq_ref[...]
    lane = lax.broadcasted_iota(jnp.int32, (rows, HEAD_SIZE), 1)
    cos_full = jnp.cos(angle)
    sine = jnp.sin(angle)
    sin_full = jnp.where(lane < HEAD_SIZE // 2, -sine, sine)
    swap = (
        lax.rem(lax.broadcasted_iota(jnp.int32, (HEAD_SIZE, HEAD_SIZE), 0) + HEAD_SIZE // 2, HEAD_SIZE)
        == lax.broadcasted_iota(jnp.int32, (HEAD_SIZE, HEAD_SIZE), 1)
    ).astype(jnp.bfloat16)

    def tables(gain_ref):
        gain = jnp.broadcast_to(gain_ref[...], (rows, HEAD_SIZE))
        return gain * cos_full, pltpu.roll(gain, HEAD_SIZE // 2, axis=1) * sin_full

    straight, crossed = tables(kg_ref)
    for g in range(groups):
        rotated = norm_rope(k_ref[:, g * HEAD_SIZE:(g + 1) * HEAD_SIZE], swap, straight, crossed)
        win_k[g, REACH] = rotated.T.astype(jnp.bfloat16)
    straight, crossed = tables(qg_ref)

    for copy in value_copies[head:]:
        copy.wait()
    for n in range(head, min(LEAD, 2 * groups)):
        own(*order[n])

    starts = jnp.broadcast_to(start_ref[...], (rows, rows)).T
    token = me * rows + lax.broadcasted_iota(jnp.int32, (rows, rows), 0)
    for b in range(REACH + 1):
        key_index = (me - REACH + b) * rows + lax.broadcasted_iota(jnp.int32, (rows, rows), 1)
        visible = (key_index >= starts) & (key_index <= token)
        hidden[b] = jnp.where(visible, 0.0, HIDDEN).astype(jnp.bfloat16)

    @pl.loop(0, jnp.maximum(REACH - me, 0))
    def _(j):
        for g in range(groups):
            win_k[g, j] = jnp.zeros((HEAD_SIZE, rows), jnp.bfloat16)
            win_v[g, j] = jnp.zeros((rows, HEAD_SIZE), jnp.bfloat16)

    weights_buf[tiles - 1][...] = jnp.zeros((blocks, tile_rows, rows), jnp.bfloat16)

    scale = HEAD_SIZE ** (-0.5) * math.log2(math.e)
    unit = (
        lax.broadcasted_iota(jnp.int32, (rows, rows), 0)
        == lax.broadcasted_iota(jnp.int32, (rows, rows), 1)
    ).astype(jnp.bfloat16)
    units = jnp.concatenate([unit] * Q_TILE, axis=0)

    def prepare(g):
        at = pl.ds(g * width, width)
        pltpu.make_async_copy(q_hbm.at[:, at], q_hbm.at[:, at], query_sem.at[g]).wait()
        for head_index in range(copies):
            q_rope[g, head_index * rows:(head_index + 1) * rows] = norm_rope(
                q_ref[g * copies + head_index], swap, straight, crossed
            ).astype(jnp.bfloat16)

    def score(g, tile):
        queries = jnp.concatenate(
            [q_rope[g, tile * tile_rows:(tile + 1) * tile_rows], units], axis=1
        )
        best = None
        for b in range(0, blocks, 2):
            pair = range(b, min(b + 2, blocks))
            keys = jnp.concatenate([
                jnp.concatenate([win_k[g, i] for i in pair], axis=1),
                jnp.concatenate([hidden[i] for i in pair], axis=1),
            ], axis=0)
            part = jnp.dot(queries, keys, preferred_element_type=jnp.float32)
            for at, i in enumerate(pair):
                piece = part[:, at * rows:(at + 1) * rows]
                scores_buf[tile % 2][i] = piece
                best = piece if best is None else jnp.maximum(best, piece)
        top = jnp.max(best, axis=1, keepdims=True)
        top_buf[tile % 2][...] = jnp.broadcast_to(top, (tile_rows, rows))

    def soften(tile):
        top = top_buf[tile % 2][...]
        for b in range(blocks):
            part = scores_buf[tile % 2][b]
            weights_buf[tile][b] = jnp.exp2((part - top) * scale).astype(jnp.bfloat16)

    def mix(g, tile):
        values = jnp.concatenate([
            win_v[g].reshape(blocks * rows, HEAD_SIZE),
            jnp.ones((blocks * rows, HEAD_SIZE), jnp.bfloat16),
        ], axis=1)
        weights = jnp.concatenate([weights_buf[tile][b] for b in range(blocks)], axis=1)
        mixed = jnp.dot(weights, values, preferred_element_type=jnp.float32)
        mixed = mixed[:, :HEAD_SIZE] / mixed[:, HEAD_SIZE:]
        for r in range(Q_TILE):
            o_ref[g * copies + tile * Q_TILE + r] = mixed[r * rows:(r + 1) * rows].astype(jnp.bfloat16)

    def result_start(g):
        for i in range(copies):
            head_index = g * copies + i
            at = pl.ds(pl.multiple_of(head_index * HEAD_SIZE, HEAD_SIZE), HEAD_SIZE)
            pltpu.make_async_copy(o_ref.at[head_index], o_hbm.at[:, at], out_sem.at[g]).start()

    def result_wait(g):
        at = pl.ds(g * width, width)
        pltpu.make_async_copy(o_hbm.at[:, at], o_hbm.at[:, at], out_sem.at[g]).wait()

    total = 2 * groups
    first_step = 16.8

    def arrival(slot, n):
        four = n + 3.4 if n < LEAD else 2 * n - LEAD + 4.4
        eight = min(2 * n + LEAD + 3.4, 2 * total + 2.4 - (total - 1 - n))
        return {4: four, 2: four + 2.9, 8: eight, 6: eight + 3.0}[slot]

    early = sorted(
        (arrival(slot, n), slot, n) for slot in (4, 2, 8, 6) for n in range(total)
    )
    late = [event for event in early if event[0] >= first_step]
    early = [event for event in early if event[0] < first_step]

    def event(slot, n):
        relay(slot, *order[n])
        if slot == 4 and n + LEAD < total:
            own(*order[n + LEAD])

    for g in range(min(2, groups)):
        prepare(g)
    ready = min(2, groups)
    for at, (_, slot, n) in enumerate(early):
        event(slot, n)
        if at % 2 == 1 and ready < groups:
            prepare(ready)
            ready += 1
    for g in range(ready, groups):
        prepare(g)

    by_tile = {}
    for when, slot, n in late:
        step = max(0, min(int(when - first_step), groups * tiles - 1))
        by_tile.setdefault(step, []).append((slot, n))

    def near(c, g):
        for slot in (1, 3, 5, 7):
            arrived(slot, c, g)

    near(KEY, 0)
    score(0, 0)

    def relays(g, tile):
        for (kind_step, todo) in by_tile.items():
            if kind_step % tiles != tile:
                continue

            @pl.when(g == kind_step // tiles)
            def _():
                for slot, n in todo:
                    event(slot, n)

    @pl.loop(0, groups - 1)
    def _(g):
        for tile in range(tiles):
            relays(g, tile)
            if tile == 0:
                near(VALUE, g)
            if tile == tiles - 1:
                near(KEY, g + 1)
                score(g + 1, 0)
            else:
                score(g, tile + 1)
            soften(tile)
            if tile == 0:
                mix(jnp.maximum(g - 1, 0), tiles - 1)

                @pl.when(g > 0)
                def _():
                    result_start(g - 1)
            else:
                mix(g, tile - 1)

    last = groups - 1
    for tile in range(tiles):
        relays(last, tile)
        if tile < tiles - 1:
            score(last, tile + 1)
        soften(tile)
        if tile == 0:
            mix(max(last - 1, 0), tiles - 1)
            if last > 0:
                result_start(last - 1)
    near(VALUE, last)
    for tile in range(tiles):
        mix(last, tile)
    result_start(last)

    for c in (KEY, VALUE):
        whole = (win_k, win_v)[c].at[:, REACH]
        for kind, (condition, _, _, target) in plan.items():
            @pl.when(condition)
            def _():
                pltpu.make_async_remote_copy(
                    src_ref=whole, dst_ref=whole, send_sem=send_sem.at[c, kind],
                    recv_sem=recv_sem.at[c, 0, 0], device_id={"sp": target}, device_id_type=MESH,
                ).wait_send()

    for g in range(groups):
        result_wait(g)


def solution(mesh):
    count = mesh.shape["sp"]

    def body(query_proj, key_projection, value_projection, query_gain, key_norm_gain, positions, doc_start):
        rows = query_proj.shape[0]
        groups = key_projection.shape[1] // HEAD_SIZE
        copies = query_proj.shape[1] // key_projection.shape[1]
        assert rows * REACH >= DOC_MAX and count % 4 == 0
        half_dim = HEAD_SIZE // 2
        inv_freq = ROPE_BASE ** (-(np.arange(half_dim) * 2.0 / HEAD_SIZE))
        freq = jnp.asarray(np.concatenate([inv_freq, inv_freq])[None, :], jnp.float32)
        blocks = REACH + 1
        tile_rows = Q_TILE * rows
        return pl.pallas_call(
            functools.partial(kernel, count, groups, copies, rows),
            out_shape=jax.ShapeDtypeStruct(query_proj.shape, jnp.bfloat16),
            in_specs=[pl.BlockSpec(memory_space=pl.ANY)] * 8,
            out_specs=pl.BlockSpec(memory_space=pl.ANY),
            scratch_shapes=[
                pltpu.VMEM((groups, blocks, HEAD_SIZE, rows), jnp.bfloat16),
                pltpu.VMEM((groups, blocks, rows, HEAD_SIZE), jnp.bfloat16),
                pltpu.VMEM((blocks, rows, rows), jnp.bfloat16),
                pltpu.VMEM((groups * copies, rows, HEAD_SIZE), jnp.bfloat16),
                pltpu.VMEM(key_projection.shape, jnp.bfloat16),
                pltpu.VMEM((groups, copies * rows, HEAD_SIZE), jnp.bfloat16),
                pltpu.VMEM((groups * copies, rows, HEAD_SIZE), jnp.bfloat16),
                pltpu.VMEM((blocks, tile_rows, rows), jnp.float32),
                pltpu.VMEM((blocks, tile_rows, rows), jnp.float32),
                pltpu.VMEM((tile_rows, rows), jnp.float32),
                pltpu.VMEM((tile_rows, rows), jnp.float32),
                pltpu.VMEM((blocks, tile_rows, rows), jnp.bfloat16),
                pltpu.VMEM((blocks, tile_rows, rows), jnp.bfloat16),
                pltpu.VMEM((blocks, tile_rows, rows), jnp.bfloat16),
                pltpu.VMEM((blocks, tile_rows, rows), jnp.bfloat16),
                pltpu.VMEM((1, HEAD_SIZE), jnp.float32),
                pltpu.VMEM((1, HEAD_SIZE), jnp.float32),
                pltpu.VMEM((1, HEAD_SIZE), jnp.float32),
                pltpu.VMEM((1, rows), jnp.int32),
                pltpu.VMEM((1, rows), jnp.int32),
                pltpu.SemaphoreType.DMA((groups,)),
                pltpu.SemaphoreType.DMA((6,)),
                pltpu.SemaphoreType.DMA((groups,)),
                pltpu.SemaphoreType.DMA((groups,)),
                pltpu.SemaphoreType.DMA((2, 10)),
                pltpu.SemaphoreType.DMA((2, REACH + 1, groups)),
            ],
            compiler_params=pltpu.CompilerParams(
                collective_id=0, has_side_effects=True, vmem_limit_bytes=60 * 1024 * 1024
            ),
        )(
            query_proj, key_projection, value_projection,
            query_gain[None, :], key_norm_gain[None, :], freq, positions[None, :], doc_start[None, :],
        )

    tokens = P(("dp", "sp"), None)
    vector = P(("dp", "sp"))
    return jax.shard_map(
        body,
        mesh=mesh,
        in_specs=(tokens, tokens, tokens, P(), P(), vector, vector),
        out_specs=tokens,
        check_vma=False,
    )
```

```python
import functools
import math

import jax
import jax.numpy as jnp
import numpy as np
from jax import lax
from jax.experimental import pallas as pl
from jax.experimental.pallas import tpu as pltpu
from jax.sharding import PartitionSpec as P

HEAD_SIZE = 128
DOC_MAX = 1024
REACH = 8
ROPE_BASE = 1000000.0
NORM_EPS = 1e-06
HIDDEN = -1e30
Q_TILE = 4
LEAD = 5
MESH = pl.DeviceIdType.MESH

KEY, VALUE = 0, 1
OWN_Z, OWN_Y, OWN_C, F4_Z, F4_Y, F4_C, F8_Y, F8_C, F2_C, F6_C = range(10)


def norm_rope(block, swap, straight, crossed):
    up = block.astype(jnp.float32)
    mean_square = jnp.mean(up * up, axis=-1, keepdims=True)
    swapped = jnp.dot(block, swap, preferred_element_type=jnp.float32)
    return (up * straight + swapped * crossed) * lax.rsqrt(mean_square + NORM_EPS)


def chunk_order(groups):
    head = min(2, groups)
    order = [(VALUE, g) for g in range(head)] + [(KEY, g) for g in range(head)]
    for g in range(head, groups):
        order += [(KEY, g), (VALUE, g)]
    return order


def kernel(
    count, groups, copies, rows,
    q_hbm, k_hbm, v_hbm, qg_hbm, kg_hbm, freq_hbm, pos_hbm, start_hbm,
    o_hbm, win_k, win_v, hidden, q_ref, k_ref, q_rope, o_ref,
    scores_a, scores_b, top_a, top_b, weights_0, weights_1,
    qg_ref, kg_ref, freq_ref, pos_ref, start_ref,
    value_sem, in_sem, query_sem, out_sem, send_sem, recv_sem,
):
    me = lax.axis_index("sp")
    core = lax.rem(me, 2)
    side = lax.rem(lax.div(me, 2), 2)
    core_peer = me + 1 - 2 * core
    side_peer = me + 2 - 4 * side
    blocks = REACH + 1
    scores_buf = [scores_a, scores_b]
    top_buf = [top_a, top_b]
    weights_buf = [weights_0, weights_1]
    tiles = copies // Q_TILE
    tile_rows = Q_TILE * rows

    def chunk(c, g, slot):
        return (win_k, win_v)[c].at[g, REACH - slot]

    def send(kind, c, g, source, target_slot, target):
        return pltpu.make_async_remote_copy(
            src_ref=chunk(c, g, source),
            dst_ref=chunk(c, g, target_slot),
            send_sem=send_sem.at[c, kind],
            recv_sem=recv_sem.at[c, target_slot, g],
            device_id={"sp": target},
            device_id_type=MESH,
        )

    has_next = me + 4 < count
    f4_slot = 6 - 4 * side

    plan = {
        OWN_Z: (has_next, 0, 4, me + 4),
        OWN_Y: (side == 0, 0, 2, side_peer),
        OWN_C: (core == 0, 0, 1, core_peer),
        F4_Z: ((me >= 4) & has_next, 4, 8, me + 4),
        F4_Y: (me >= 4, 4, f4_slot, side_peer),
        F4_C: (me >= 4, 4, 5 - 2 * core, core_peer),
        F8_Y: ((me >= 8) & (side == 1), 8, 6, side_peer),
        F8_C: ((me >= 8) & (core == 1), 8, 7, core_peer),
        F2_C: (me >= 2, 2, 3 - 2 * core, core_peer),
        F6_C: (me >= 6, 6, 7 - 2 * core, core_peer),
    }

    def start(kind, c, g):
        condition, source, target_slot, target = plan[kind]

        @pl.when(condition)
        def _():
            send(kind, c, g, source, target_slot, target).start()

    def arrived(slot, c, g):
        @pl.when(me >= slot)
        def _():
            send(OWN_Z, c, g, 0, slot, me).wait_recv()

    def own(c, g):
        for kind in (OWN_Z, OWN_Y, OWN_C):
            start(kind, c, g)

    forwards = {4: (F4_Z, F4_Y, F4_C), 8: (F8_Y, F8_C), 2: (F2_C,), 6: (F6_C,)}

    def relay(slot, c, g):
        arrived(slot, c, g)
        for kind in forwards[slot]:
            start(kind, c, g)

    value_copies = [
        pltpu.make_async_copy(
            v_hbm.at[:, pl.ds(g * HEAD_SIZE, HEAD_SIZE)],
            win_v.at[g, REACH],
            value_sem.at[g],
        )
        for g in range(groups)
    ]
    small = [
        pltpu.make_async_copy(source, target, in_sem.at[i])
        for i, (source, target) in enumerate([
            (pos_hbm, pos_ref), (freq_hbm, freq_ref), (kg_hbm, kg_ref), (k_hbm, k_ref),
            (start_hbm, start_ref), (qg_hbm, qg_ref),
        ])
    ]
    width = copies * HEAD_SIZE
    query_copies = [
        pltpu.make_async_copy(
            q_hbm.at[:, pl.ds(i * HEAD_SIZE, HEAD_SIZE)], q_ref.at[i], query_sem.at[i // copies]
        )
        for i in range(groups * copies)
    ]
    barrier = pltpu.get_barrier_semaphore()
    for peer in (core_peer, side_peer):
        pl.semaphore_signal(barrier, inc=1, device_id={"sp": peer}, device_id_type=MESH)

    @pl.when(has_next)
    def _():
        pl.semaphore_signal(barrier, inc=1, device_id={"sp": me + 4}, device_id_type=MESH)

    @pl.when(me >= 4)
    def _():
        pl.semaphore_signal(barrier, inc=1, device_id={"sp": me - 4}, device_id_type=MESH)

    for copy in value_copies[:2] + small + value_copies[2:] + query_copies:
        copy.start()

    order = chunk_order(groups)
    head = min(2, groups)
    for copy in value_copies[:head]:
        copy.wait()
    inner = (me >= 4) & has_next

    @pl.when(inner)
    def _():
        pl.semaphore_wait(barrier, 4)

    @pl.when(jnp.logical_not(inner))
    def _():
        pl.semaphore_wait(barrier, 3 if count > 4 else 2)

    for n in range(head):
        own(*order[n])

    for copy in small:
        copy.wait()
    places = jnp.broadcast_to(pos_ref[...].astype(jnp.float32), (HEAD_SIZE, rows)).T
    angle = places * freq_ref[...]
    lane = lax.broadcasted_iota(jnp.int32, (rows, HEAD_SIZE), 1)
    cos_full = jnp.cos(angle)
    sine = jnp.sin(angle)
    sin_full = jnp.where(lane < HEAD_SIZE // 2, -sine, sine)
    swap = (
        lax.rem(lax.broadcasted_iota(jnp.int32, (HEAD_SIZE, HEAD_SIZE), 0) + HEAD_SIZE // 2, HEAD_SIZE)
        == lax.broadcasted_iota(jnp.int32, (HEAD_SIZE, HEAD_SIZE), 1)
    ).astype(jnp.bfloat16)

    def tables(gain_ref):
        gain = jnp.broadcast_to(gain_ref[...], (rows, HEAD_SIZE))
        return gain * cos_full, pltpu.roll(gain, HEAD_SIZE // 2, axis=1) * sin_full

    straight, crossed = tables(kg_ref)
    for g in range(groups):
        rotated = norm_rope(k_ref[:, g * HEAD_SIZE:(g + 1) * HEAD_SIZE], swap, straight, crossed)
        win_k[g, REACH] = rotated.T.astype(jnp.bfloat16)
    straight, crossed = tables(qg_ref)

    for copy in value_copies[head:]:
        copy.wait()
    for n in range(head, min(LEAD, 2 * groups)):
        own(*order[n])

    starts = jnp.broadcast_to(start_ref[...], (rows, rows)).T
    token = me * rows + lax.broadcasted_iota(jnp.int32, (rows, rows), 0)
    for b in range(REACH + 1):
        key_index = (me - REACH + b) * rows + lax.broadcasted_iota(jnp.int32, (rows, rows), 1)
        visible = (key_index >= starts) & (key_index <= token)
        hidden[b] = jnp.where(visible, 0.0, HIDDEN).astype(jnp.bfloat16)

    @pl.loop(0, jnp.maximum(REACH - me, 0))
    def _(j):
        for g in range(groups):
            win_k[g, j] = jnp.zeros((HEAD_SIZE, rows), jnp.bfloat16)
            win_v[g, j] = jnp.zeros((rows, HEAD_SIZE), jnp.bfloat16)

    weights_buf[tiles - 1][...] = jnp.zeros((blocks, tile_rows, rows), jnp.bfloat16)

    scale = HEAD_SIZE ** (-0.5) * math.log2(math.e)
    unit = (
        lax.broadcasted_iota(jnp.int32, (rows, rows), 0)
        == lax.broadcasted_iota(jnp.int32, (rows, rows), 1)
    ).astype(jnp.bfloat16)
    units = jnp.concatenate([unit] * Q_TILE, axis=0)

    def prepare(g):
        at = pl.ds(g * width, width)
        pltpu.make_async_copy(q_hbm.at[:, at], q_hbm.at[:, at], query_sem.at[g]).wait()
        for head_index in range(copies):
            q_rope[g, head_index * rows:(head_index + 1) * rows] = norm_rope(
                q_ref[g * copies + head_index], swap, straight, crossed
            ).astype(jnp.bfloat16)

    def score(g, tile):
        queries = jnp.concatenate(
            [q_rope[g, tile * tile_rows:(tile + 1) * tile_rows], units], axis=1
        )
        best = None
        for b in range(0, blocks, 2):
            pair = range(b, min(b + 2, blocks))
            keys = jnp.concatenate([
                jnp.concatenate([win_k[g, i] for i in pair], axis=1),
                jnp.concatenate([hidden[i] for i in pair], axis=1),
            ], axis=0)
            part = jnp.dot(queries, keys, preferred_element_type=jnp.float32)
            for at, i in enumerate(pair):
                piece = part[:, at * rows:(at + 1) * rows]
                scores_buf[tile % 2][i] = piece
                best = piece if best is None else jnp.maximum(best, piece)
        top_buf[tile % 2][...] = best

    def soften(tile):
        top = jnp.max(top_buf[tile % 2][...], axis=1, keepdims=True)
        for b in range(blocks):
            part = scores_buf[tile % 2][b]
            weights_buf[tile][b] = jnp.exp2((part - top) * scale).astype(jnp.bfloat16)

    def mix(g, tile):
        values = jnp.concatenate([
            win_v[g].reshape(blocks * rows, HEAD_SIZE),
            jnp.ones((blocks * rows, HEAD_SIZE), jnp.bfloat16),
        ], axis=1)
        weights = jnp.concatenate([weights_buf[tile][b] for b in range(blocks)], axis=1)
        mixed = jnp.dot(weights, values, preferred_element_type=jnp.float32)
        mixed = mixed[:, :HEAD_SIZE] / mixed[:, HEAD_SIZE:]
        for r in range(Q_TILE):
            o_ref[g * copies + tile * Q_TILE + r] = mixed[r * rows:(r + 1) * rows].astype(jnp.bfloat16)

    def result_start(g):
        for i in range(copies):
            head_index = g * copies + i
            at = pl.ds(pl.multiple_of(head_index * HEAD_SIZE, HEAD_SIZE), HEAD_SIZE)
            pltpu.make_async_copy(o_ref.at[head_index], o_hbm.at[:, at], out_sem.at[g]).start()

    def result_wait(g):
        at = pl.ds(g * width, width)
        pltpu.make_async_copy(o_hbm.at[:, at], o_hbm.at[:, at], out_sem.at[g]).wait()

    total = 2 * groups
    first_step = 16.8

    def arrival(slot, n):
        four = n + 3.4 if n < LEAD else 2 * n - LEAD + 4.4
        eight = min(2 * n + LEAD + 3.4, 2 * total + 2.4 - (total - 1 - n))
        return {4: four, 2: four + 2.9, 8: eight, 6: eight + 3.0}[slot]

    early = sorted(
        (arrival(slot, n), slot, n) for slot in (4, 2, 8, 6) for n in range(total)
    )
    late = [event for event in early if event[0] >= first_step]
    early = [event for event in early if event[0] < first_step]

    def event(slot, n):
        relay(slot, *order[n])
        if slot == 4 and n + LEAD < total:
            own(*order[n + LEAD])

    for g in range(min(2, groups)):
        prepare(g)
    ready = min(2, groups)
    for at, (_, slot, n) in enumerate(early):
        event(slot, n)
        if at % 2 == 1 and ready < groups:
            prepare(ready)
            ready += 1
    for g in range(ready, groups):
        prepare(g)

    by_tile = {}
    for when, slot, n in late:
        step = max(0, min(int((when - first_step) * tiles / 4), groups * tiles - 1))
        by_tile.setdefault(step, []).append((slot, n))

    def near(c, g):
        for slot in (1, 3, 5, 7):
            arrived(slot, c, g)

    near(VALUE, 0)
    near(KEY, 0)
    score(0, 0)

    def relays(g, tile):
        for (kind_step, todo) in by_tile.items():
            if kind_step % tiles != tile:
                continue

            @pl.when(g == kind_step // tiles)
            def _():
                for slot, n in todo:
                    event(slot, n)

    @pl.loop(0, groups - 1)
    def _(g):
        for tile in range(tiles):
            relays(g, tile)
            if tile == 1:
                @pl.when(g > 0)
                def _():
                    near(VALUE, g)
            if tile == tiles - 1:
                near(KEY, g + 1)
                score(g + 1, 0)
            else:
                score(g, tile + 1)
            soften(tile)
            if tile == 0:
                mix(jnp.maximum(g - 1, 0), tiles - 1)

                @pl.when(g > 0)
                def _():
                    result_start(g - 1)
            else:
                mix(g, tile - 1)

    last = groups - 1
    for tile in range(tiles):
        relays(last, tile)
        if tile < tiles - 1:
            score(last, tile + 1)
        soften(tile)
        if tile == 0:
            mix(max(last - 1, 0), tiles - 1)
            if last > 0:
                result_start(last - 1)
    near(VALUE, last)
    for tile in range(tiles):
        mix(last, tile)
    result_start(last)

    for c in (KEY, VALUE):
        whole = (win_k, win_v)[c].at[:, REACH]
        for kind, (condition, _, _, target) in plan.items():
            @pl.when(condition)
            def _():
                pltpu.make_async_remote_copy(
                    src_ref=whole, dst_ref=whole, send_sem=send_sem.at[c, kind],
                    recv_sem=recv_sem.at[c, 0, 0], device_id={"sp": target}, device_id_type=MESH,
                ).wait_send()

    for g in range(groups):
        result_wait(g)


def solution(mesh):
    count = mesh.shape["sp"]

    def body(query_proj, key_projection, value_projection, query_gain, key_norm_gain, positions, doc_start):
        rows = query_proj.shape[0]
        groups = key_projection.shape[1] // HEAD_SIZE
        copies = query_proj.shape[1] // key_projection.shape[1]
        assert rows * REACH >= DOC_MAX and count % 4 == 0
        half_dim = HEAD_SIZE // 2
        inv_freq = ROPE_BASE ** (-(np.arange(half_dim) * 2.0 / HEAD_SIZE))
        freq = jnp.asarray(np.concatenate([inv_freq, inv_freq])[None, :], jnp.float32)
        blocks = REACH + 1
        tile_rows = Q_TILE * rows
        return pl.pallas_call(
            functools.partial(kernel, count, groups, copies, rows),
            out_shape=jax.ShapeDtypeStruct(query_proj.shape, jnp.bfloat16),
            in_specs=[pl.BlockSpec(memory_space=pl.ANY)] * 8,
            out_specs=pl.BlockSpec(memory_space=pl.ANY),
            scratch_shapes=[
                pltpu.VMEM((groups, blocks, HEAD_SIZE, rows), jnp.bfloat16),
                pltpu.VMEM((groups, blocks, rows, HEAD_SIZE), jnp.bfloat16),
                pltpu.VMEM((blocks, rows, rows), jnp.bfloat16),
                pltpu.VMEM((groups * copies, rows, HEAD_SIZE), jnp.bfloat16),
                pltpu.VMEM(key_projection.shape, jnp.bfloat16),
                pltpu.VMEM((groups, copies * rows, HEAD_SIZE), jnp.bfloat16),
                pltpu.VMEM((groups * copies, rows, HEAD_SIZE), jnp.bfloat16),
                pltpu.VMEM((blocks, tile_rows, rows), jnp.float32),
                pltpu.VMEM((blocks, tile_rows, rows), jnp.float32),
                pltpu.VMEM((tile_rows, rows), jnp.float32),
                pltpu.VMEM((tile_rows, rows), jnp.float32),
                pltpu.VMEM((blocks, tile_rows, rows), jnp.bfloat16),
                pltpu.VMEM((blocks, tile_rows, rows), jnp.bfloat16),
                pltpu.VMEM((1, HEAD_SIZE), jnp.float32),
                pltpu.VMEM((1, HEAD_SIZE), jnp.float32),
                pltpu.VMEM((1, HEAD_SIZE), jnp.float32),
                pltpu.VMEM((1, rows), jnp.int32),
                pltpu.VMEM((1, rows), jnp.int32),
                pltpu.SemaphoreType.DMA((groups,)),
                pltpu.SemaphoreType.DMA((6,)),
                pltpu.SemaphoreType.DMA((groups,)),
                pltpu.SemaphoreType.DMA((groups,)),
                pltpu.SemaphoreType.DMA((2, 10)),
                pltpu.SemaphoreType.DMA((2, REACH + 1, groups)),
            ],
            compiler_params=pltpu.CompilerParams(
                collective_id=0, has_side_effects=True, vmem_limit_bytes=60 * 1024 * 1024
            ),
        )(
            query_proj, key_projection, value_projection,
            query_gain[None, :], key_norm_gain[None, :], freq, positions[None, :], doc_start[None, :],
        )

    tokens = P(("dp", "sp"), None)
    vector = P(("dp", "sp"))
    return jax.shard_map(
        body,
        mesh=mesh,
        in_specs=(tokens, tokens, tokens, P(), P(), vector, vector),
        out_specs=tokens,
        check_vma=False,
    )
```

```python
import functools
import math

import jax
import jax.numpy as jnp
import numpy as np
from jax import lax
from jax.experimental import pallas as pl
from jax.experimental.pallas import tpu as pltpu
from jax.sharding import PartitionSpec as P

HEAD_SIZE = 128
DOC_MAX = 1024
REACH = 8
ROPE_BASE = 1000000.0
NORM_EPS = 1e-06
HIDDEN = -1e30
Q_TILE = 4
LEAD = 5
MESH = pl.DeviceIdType.MESH

KEY, VALUE = 0, 1
OWN_Z, OWN_Y, OWN_C, F4_Z, F4_Y, F4_C, F8_Y, F8_C, F2_C, F6_C = range(10)


def norm_rope(block, swap, straight, crossed):
    up = block.astype(jnp.float32)
    mean_square = jnp.mean(up * up, axis=-1, keepdims=True)
    swapped = jnp.dot(block, swap, preferred_element_type=jnp.float32)
    return (up * straight + swapped * crossed) * lax.rsqrt(mean_square + NORM_EPS)


def chunk_order(groups):
    head = min(2, groups)
    order = [(VALUE, g) for g in range(head)] + [(KEY, g) for g in range(head)]
    for g in range(head, groups):
        order += [(KEY, g), (VALUE, g)]
    return order


def kernel(
    count, groups, copies, rows,
    q_hbm, k_hbm, v_hbm, qg_hbm, kg_hbm, freq_hbm, pos_hbm, start_hbm,
    o_ref, win_k, win_v, hidden, q_ref, k_ref, q_rope,
    scores_a, scores_b, top_a, top_b, weights_0, weights_1,
    qg_ref, kg_ref, freq_ref, pos_ref, start_ref,
    value_sem, in_sem, query_sem, send_sem, recv_sem,
):
    me = lax.axis_index("sp")
    core = lax.rem(me, 2)
    side = lax.rem(lax.div(me, 2), 2)
    core_peer = me + 1 - 2 * core
    side_peer = me + 2 - 4 * side
    blocks = REACH + 1
    scores_buf = [scores_a, scores_b]
    top_buf = [top_a, top_b]
    weights_buf = [weights_0, weights_1]
    tiles = copies // Q_TILE
    tile_rows = Q_TILE * rows

    def chunk(c, g, slot):
        return (win_k, win_v)[c].at[g, REACH - slot]

    def send(kind, c, g, source, target_slot, target):
        return pltpu.make_async_remote_copy(
            src_ref=chunk(c, g, source),
            dst_ref=chunk(c, g, target_slot),
            send_sem=send_sem.at[c, kind],
            recv_sem=recv_sem.at[c, target_slot, g],
            device_id={"sp": target},
            device_id_type=MESH,
        )

    has_next = me + 4 < count
    f4_slot = 6 - 4 * side

    plan = {
        OWN_Z: (has_next, 0, 4, me + 4),
        OWN_Y: (side == 0, 0, 2, side_peer),
        OWN_C: (core == 0, 0, 1, core_peer),
        F4_Z: ((me >= 4) & has_next, 4, 8, me + 4),
        F4_Y: (me >= 4, 4, f4_slot, side_peer),
        F4_C: (me >= 4, 4, 5 - 2 * core, core_peer),
        F8_Y: ((me >= 8) & (side == 1), 8, 6, side_peer),
        F8_C: ((me >= 8) & (core == 1), 8, 7, core_peer),
        F2_C: (me >= 2, 2, 3 - 2 * core, core_peer),
        F6_C: (me >= 6, 6, 7 - 2 * core, core_peer),
    }

    def start(kind, c, g):
        condition, source, target_slot, target = plan[kind]

        @pl.when(condition)
        def _():
            send(kind, c, g, source, target_slot, target).start()

    def arrived(slot, c, g):
        @pl.when(me >= slot)
        def _():
            send(OWN_Z, c, g, 0, slot, me).wait_recv()

    def own(c, g):
        for kind in (OWN_Z, OWN_Y, OWN_C):
            start(kind, c, g)

    forwards = {4: (F4_Z, F4_Y, F4_C), 8: (F8_Y, F8_C), 2: (F2_C,), 6: (F6_C,)}

    def relay(slot, c, g):
        arrived(slot, c, g)
        for kind in forwards[slot]:
            start(kind, c, g)

    value_copies = [
        pltpu.make_async_copy(
            v_hbm.at[:, pl.ds(g * HEAD_SIZE, HEAD_SIZE)],
            win_v.at[g, REACH],
            value_sem.at[g],
        )
        for g in range(groups)
    ]
    small = [
        pltpu.make_async_copy(source, target, in_sem.at[i])
        for i, (source, target) in enumerate([
            (pos_hbm, pos_ref), (freq_hbm, freq_ref), (kg_hbm, kg_ref), (k_hbm, k_ref),
            (start_hbm, start_ref), (qg_hbm, qg_ref),
        ])
    ]
    width = copies * HEAD_SIZE
    query_copies = [
        pltpu.make_async_copy(
            q_hbm.at[:, pl.ds(i * HEAD_SIZE, HEAD_SIZE)], q_ref.at[i], query_sem.at[i // copies]
        )
        for i in range(groups * copies)
    ]
    barrier = pltpu.get_barrier_semaphore()
    for peer in (core_peer, side_peer):
        pl.semaphore_signal(barrier, inc=1, device_id={"sp": peer}, device_id_type=MESH)

    @pl.when(has_next)
    def _():
        pl.semaphore_signal(barrier, inc=1, device_id={"sp": me + 4}, device_id_type=MESH)

    @pl.when(me >= 4)
    def _():
        pl.semaphore_signal(barrier, inc=1, device_id={"sp": me - 4}, device_id_type=MESH)

    for copy in value_copies[:2] + small + value_copies[2:] + query_copies:
        copy.start()

    order = chunk_order(groups)
    head = min(2, groups)
    for copy in value_copies[:head]:
        copy.wait()
    inner = (me >= 4) & has_next

    @pl.when(inner)
    def _():
        pl.semaphore_wait(barrier, 4)

    @pl.when(jnp.logical_not(inner))
    def _():
        pl.semaphore_wait(barrier, 3 if count > 4 else 2)

    for n in range(head):
        own(*order[n])

    for copy in small:
        copy.wait()
    places = jnp.broadcast_to(pos_ref[...].astype(jnp.float32), (HEAD_SIZE, rows)).T
    angle = places * freq_ref[...]
    lane = lax.broadcasted_iota(jnp.int32, (rows, HEAD_SIZE), 1)
    cos_full = jnp.cos(angle)
    sine = jnp.sin(angle)
    sin_full = jnp.where(lane < HEAD_SIZE // 2, -sine, sine)
    swap = (
        lax.rem(lax.broadcasted_iota(jnp.int32, (HEAD_SIZE, HEAD_SIZE), 0) + HEAD_SIZE // 2, HEAD_SIZE)
        == lax.broadcasted_iota(jnp.int32, (HEAD_SIZE, HEAD_SIZE), 1)
    ).astype(jnp.bfloat16)

    def tables(gain_ref):
        gain = jnp.broadcast_to(gain_ref[...], (rows, HEAD_SIZE))
        return gain * cos_full, pltpu.roll(gain, HEAD_SIZE // 2, axis=1) * sin_full

    straight, crossed = tables(kg_ref)
    for g in range(groups):
        rotated = norm_rope(k_ref[:, g * HEAD_SIZE:(g + 1) * HEAD_SIZE], swap, straight, crossed)
        win_k[g, REACH] = rotated.T.astype(jnp.bfloat16)
    straight, crossed = tables(qg_ref)

    for copy in value_copies[head:]:
        copy.wait()
    for n in range(head, min(LEAD, 2 * groups)):
        own(*order[n])

    starts = jnp.broadcast_to(start_ref[...], (rows, rows)).T
    token = me * rows + lax.broadcasted_iota(jnp.int32, (rows, rows), 0)
    for b in range(REACH + 1):
        key_index = (me - REACH + b) * rows + lax.broadcasted_iota(jnp.int32, (rows, rows), 1)
        visible = (key_index >= starts) & (key_index <= token)
        hidden[b] = jnp.where(visible, 0.0, HIDDEN).astype(jnp.bfloat16)

    @pl.loop(0, jnp.maximum(REACH - me, 0))
    def _(j):
        for g in range(groups):
            win_k[g, j] = jnp.zeros((HEAD_SIZE, rows), jnp.bfloat16)
            win_v[g, j] = jnp.zeros((rows, HEAD_SIZE), jnp.bfloat16)

    weights_buf[tiles - 1][...] = jnp.zeros((blocks, tile_rows, rows), jnp.bfloat16)

    scale = HEAD_SIZE ** (-0.5) * math.log2(math.e)
    unit = (
        lax.broadcasted_iota(jnp.int32, (rows, rows), 0)
        == lax.broadcasted_iota(jnp.int32, (rows, rows), 1)
    ).astype(jnp.bfloat16)
    units = jnp.concatenate([unit] * Q_TILE, axis=0)

    def prepare(g):
        at = pl.ds(g * width, width)
        pltpu.make_async_copy(q_hbm.at[:, at], q_hbm.at[:, at], query_sem.at[g]).wait()
        for head_index in range(copies):
            q_rope[g, head_index * rows:(head_index + 1) * rows] = norm_rope(
                q_ref[g * copies + head_index], swap, straight, crossed
            ).astype(jnp.bfloat16)

    def score(g, tile):
        queries = jnp.concatenate(
            [q_rope[g, tile * tile_rows:(tile + 1) * tile_rows], units], axis=1
        )
        best = None
        for b in range(0, blocks, 2):
            pair = range(b, min(b + 2, blocks))
            keys = jnp.concatenate([
                jnp.concatenate([win_k[g, i] for i in pair], axis=1),
                jnp.concatenate([hidden[i] for i in pair], axis=1),
            ], axis=0)
            part = jnp.dot(queries, keys, preferred_element_type=jnp.float32)
            for at, i in enumerate(pair):
                piece = part[:, at * rows:(at + 1) * rows]
                scores_buf[tile % 2][i] = piece
                best = piece if best is None else jnp.maximum(best, piece)
        top_buf[tile % 2][...] = best

    def soften(tile):
        top = jnp.max(top_buf[tile % 2][...], axis=1, keepdims=True)
        for b in range(blocks):
            part = scores_buf[tile % 2][b]
            weights_buf[tile][b] = jnp.exp2((part - top) * scale).astype(jnp.bfloat16)

    def mix(g, tile):
        values = jnp.concatenate([
            win_v[g].reshape(blocks * rows, HEAD_SIZE),
            jnp.ones((blocks * rows, HEAD_SIZE), jnp.bfloat16),
        ], axis=1)
        weights = jnp.concatenate([weights_buf[tile][b] for b in range(blocks)], axis=1)
        mixed = jnp.dot(weights, values, preferred_element_type=jnp.float32)
        mixed = mixed[:, :HEAD_SIZE] / mixed[:, HEAD_SIZE:]
        for r in range(Q_TILE):
            o_ref[g * copies + tile * Q_TILE + r] = mixed[r * rows:(r + 1) * rows].astype(jnp.bfloat16)

    total = 2 * groups
    first_step = 16.8

    def arrival(slot, n):
        four = n + 3.4 if n < LEAD else 2 * n - LEAD + 4.4
        eight = min(2 * n + LEAD + 3.4, 2 * total + 2.4 - (total - 1 - n))
        return {4: four, 2: four + 2.9, 8: eight, 6: eight + 3.0}[slot]

    early = sorted(
        (arrival(slot, n), slot, n) for slot in (4, 2, 8, 6) for n in range(total)
    )
    late = [event for event in early if event[0] >= first_step]
    early = [event for event in early if event[0] < first_step]

    def event(slot, n):
        relay(slot, *order[n])
        if slot == 4 and n + LEAD < total:
            own(*order[n + LEAD])

    for g in range(min(2, groups)):
        prepare(g)
    ready = min(2, groups)
    for at, (_, slot, n) in enumerate(early):
        event(slot, n)
        if at % 2 == 1 and ready < groups:
            prepare(ready)
            ready += 1
    for g in range(ready, groups):
        prepare(g)

    by_tile = {}
    for when, slot, n in late:
        step = max(0, min(int((when - first_step) * tiles / 4), groups * tiles - 1))
        by_tile.setdefault(step, []).append((slot, n))

    def near(c, g):
        for slot in (1, 3, 5, 7):
            arrived(slot, c, g)

    near(VALUE, 0)
    near(KEY, 0)
    score(0, 0)

    def relays(g, tile):
        for (kind_step, todo) in by_tile.items():
            if kind_step % tiles != tile:
                continue

            @pl.when(g == kind_step // tiles)
            def _():
                for slot, n in todo:
                    event(slot, n)

    @pl.loop(0, groups - 1)
    def _(g):
        for tile in range(tiles):
            relays(g, tile)
            if tile == 1:
                @pl.when(g > 0)
                def _():
                    near(VALUE, g)
            if tile == tiles - 1:
                near(KEY, g + 1)
                score(g + 1, 0)
            else:
                score(g, tile + 1)
            soften(tile)
            if tile == 0:
                mix(jnp.maximum(g - 1, 0), tiles - 1)
            else:
                mix(g, tile - 1)

    last = groups - 1
    for tile in range(tiles):
        relays(last, tile)
        if tile < tiles - 1:
            score(last, tile + 1)
        soften(tile)
        if tile == 0:
            mix(max(last - 1, 0), tiles - 1)
    near(VALUE, last)
    for tile in range(tiles):
        mix(last, tile)

    for c in (KEY, VALUE):
        whole = (win_k, win_v)[c].at[:, REACH]
        for kind, (condition, _, _, target) in plan.items():
            @pl.when(condition)
            def _():
                pltpu.make_async_remote_copy(
                    src_ref=whole, dst_ref=whole, send_sem=send_sem.at[c, kind],
                    recv_sem=recv_sem.at[c, 0, 0], device_id={"sp": target}, device_id_type=MESH,
                ).wait_send()


def leave(heads_ref, o_hbm, sem):
    for i in range(heads_ref.shape[0]):
        at = pl.ds(i * HEAD_SIZE, HEAD_SIZE)
        pltpu.make_async_copy(heads_ref.at[i], o_hbm.at[:, at], sem).start()
    pltpu.make_async_copy(o_hbm, o_hbm, sem).wait()


def solution(mesh):
    count = mesh.shape["sp"]

    def body(query_proj, key_projection, value_projection, query_gain, key_norm_gain, positions, doc_start):
        rows = query_proj.shape[0]
        groups = key_projection.shape[1] // HEAD_SIZE
        copies = query_proj.shape[1] // key_projection.shape[1]
        assert rows * REACH >= DOC_MAX and count % 4 == 0
        half_dim = HEAD_SIZE // 2
        inv_freq = ROPE_BASE ** (-(np.arange(half_dim) * 2.0 / HEAD_SIZE))
        freq = jnp.asarray(np.concatenate([inv_freq, inv_freq])[None, :], jnp.float32)
        blocks = REACH + 1
        tile_rows = Q_TILE * rows
        heads = pl.pallas_call(
            functools.partial(kernel, count, groups, copies, rows),
            out_shape=jax.ShapeDtypeStruct((groups * copies, rows, HEAD_SIZE), jnp.bfloat16),
            in_specs=[pl.BlockSpec(memory_space=pl.ANY)] * 8,
            out_specs=pl.BlockSpec(memory_space=pltpu.VMEM),
            scratch_shapes=[
                pltpu.VMEM((groups, blocks, HEAD_SIZE, rows), jnp.bfloat16),
                pltpu.VMEM((groups, blocks, rows, HEAD_SIZE), jnp.bfloat16),
                pltpu.VMEM((blocks, rows, rows), jnp.bfloat16),
                pltpu.VMEM((groups * copies, rows, HEAD_SIZE), jnp.bfloat16),
                pltpu.VMEM(key_projection.shape, jnp.bfloat16),
                pltpu.VMEM((groups, copies * rows, HEAD_SIZE), jnp.bfloat16),
                pltpu.VMEM((blocks, tile_rows, rows), jnp.float32),
                pltpu.VMEM((blocks, tile_rows, rows), jnp.float32),
                pltpu.VMEM((tile_rows, rows), jnp.float32),
                pltpu.VMEM((tile_rows, rows), jnp.float32),
                pltpu.VMEM((blocks, tile_rows, rows), jnp.bfloat16),
                pltpu.VMEM((blocks, tile_rows, rows), jnp.bfloat16),
                pltpu.VMEM((1, HEAD_SIZE), jnp.float32),
                pltpu.VMEM((1, HEAD_SIZE), jnp.float32),
                pltpu.VMEM((1, HEAD_SIZE), jnp.float32),
                pltpu.VMEM((1, rows), jnp.int32),
                pltpu.VMEM((1, rows), jnp.int32),
                pltpu.SemaphoreType.DMA((groups,)),
                pltpu.SemaphoreType.DMA((6,)),
                pltpu.SemaphoreType.DMA((groups,)),
                pltpu.SemaphoreType.DMA((2, 10)),
                pltpu.SemaphoreType.DMA((2, REACH + 1, groups)),
            ],
            compiler_params=pltpu.CompilerParams(
                collective_id=0, has_side_effects=True, vmem_limit_bytes=41943040
            ),
        )(
            *(pltpu.with_memory_space_constraint(array, pltpu.HBM) for array in (
                query_proj, key_projection, value_projection,
                query_gain[None, :], key_norm_gain[None, :], freq, positions[None, :], doc_start[None, :],
            ))
        )
        return pl.pallas_call(
            leave,
            out_shape=jax.ShapeDtypeStruct(query_proj.shape, jnp.bfloat16),
            in_specs=[pl.BlockSpec(memory_space=pltpu.VMEM)],
            out_specs=pl.BlockSpec(memory_space=pl.ANY),
            scratch_shapes=[pltpu.SemaphoreType.DMA],
            compiler_params=pltpu.CompilerParams(vmem_limit_bytes=8 * 1024 * 1024),
        )(heads)

    tokens = P(("dp", "sp"), None)
    vector = P(("dp", "sp"))
    return jax.shard_map(
        body,
        mesh=mesh,
        in_specs=(tokens, tokens, tokens, P(), P(), vector, vector),
        out_specs=tokens,
        check_vma=False,
    )
```

```python
import functools
import math

import jax
import jax.numpy as jnp
import numpy as np
from jax import lax
from jax.experimental import pallas as pl
from jax.experimental.pallas import tpu as pltpu
from jax.sharding import PartitionSpec as P

HEAD_SIZE = 128
DOC_MAX = 1024
REACH = 8
ROPE_BASE = 1000000.0
NORM_EPS = 1e-06
HIDDEN = -1e30
Q_TILE = 4
BLOCK_STEP = 2.1
MESH = pl.DeviceIdType.MESH

KEY, VALUE, BOTH = 0, 1, 2
OWN_Z, OWN_Y, OWN_C, F4_Z, F4_Y, F4_C, F8_Y, F8_C, F2_C, F6_C = range(10)
CHIP_KINDS = (OWN_Z, OWN_Y, F4_Z, F4_Y, F8_Y)


def norm_rope(block, swap, straight, crossed):
    up = block.astype(jnp.float32)
    mean_square = jnp.mean(up * up, axis=-1, keepdims=True)
    swapped = jnp.dot(block, swap, preferred_element_type=jnp.float32)
    return (up * straight + swapped * crossed) * lax.rsqrt(mean_square + NORM_EPS)


def chunk_order(groups):
    middle = [(BOTH, g) for g in range(1, groups - 1)]
    return [(VALUE, 0), (KEY, 0)] + middle + [(KEY, groups - 1), (VALUE, groups - 1)]


def expected_arrivals(sizes):
    total = len(sizes)
    line = [("own", n) for n in range(3)] + [("far", 0)]
    for n in range(1, total):
        line += [("far", n)] + ([("own", n + 2)] if n + 2 < total else [])
    at, end = 0.0, {}
    for item in line:
        at += sizes[item[1]]
        end[item] = at
    arrivals = []
    for n, size in enumerate(sizes):
        four, eight = end["own", n] + 2.7, end["far", n] + 2.7
        hop = size + 3.6
        arrivals += [(four, 4, n), (four + hop, 2, n), (eight, 8, n), (eight + hop, 6, n)]
    return sorted(arrivals)


def kernel(
    count, groups, copies, rows,
    q_hbm, k_hbm, v_hbm, qg_hbm, kg_hbm, freq_hbm, pos_hbm, start_hbm,
    o_ref, win, hidden, q_ref, k_ref, q_rope,
    scores_a, scores_b, top_a, top_b, weights_0, weights_1,
    qg_ref, kg_ref, freq_ref, pos_ref, start_ref,
    value_sem, in_sem, query_sem, send_sem, recv_sem,
):
    me = lax.axis_index("sp")
    core = lax.rem(me, 2)
    side = lax.rem(lax.div(me, 2), 2)
    core_peer = me + 1 - 2 * core
    side_peer = me + 2 - 4 * side
    blocks = REACH + 1
    scores_buf = [scores_a, scores_b]
    top_buf = [top_a, top_b]
    weights_buf = [weights_0, weights_1]
    tiles = copies // Q_TILE
    tile_rows = Q_TILE * rows

    order = chunk_order(groups)
    total = len(order)

    def chunk(n, slot):
        kind, g = order[n]
        if kind == BOTH:
            return win.at[g, REACH - slot]
        return win.at[g, REACH - slot, kind]

    def send(kind, n, source, target_slot, target):
        return pltpu.make_async_remote_copy(
            src_ref=chunk(n, source),
            dst_ref=chunk(n, target_slot),
            send_sem=send_sem.at[kind],
            recv_sem=recv_sem.at[target_slot // 2 if kind in CHIP_KINDS else 0, n],
            device_id={"sp": target},
            device_id_type=MESH,
        )

    has_next = me + 4 < count
    f4_slot = 6 - 4 * side

    plan = {
        OWN_Z: (has_next, 0, 4, me + 4),
        OWN_Y: (side == 0, 0, 2, side_peer),
        OWN_C: (core == 0, 0, 1, core_peer),
        F4_Z: ((me >= 4) & has_next, 4, 8, me + 4),
        F4_Y: (me >= 4, 4, f4_slot, side_peer),
        F4_C: (me >= 4, 4, 5 - 2 * core, core_peer),
        F8_Y: ((me >= 8) & (side == 1), 8, 6, side_peer),
        F8_C: ((me >= 8) & (core == 1), 8, 7, core_peer),
        F2_C: (me >= 2, 2, 3 - 2 * core, core_peer),
        F6_C: (me >= 6, 6, 7 - 2 * core, core_peer),
    }

    def start(kind, n):
        condition, source, target_slot, target = plan[kind]

        @pl.when(condition)
        def _():
            send(kind, n, source, target_slot, target).start()

    def landed(ref, sem):
        pltpu.make_async_remote_copy(
            src_ref=ref, dst_ref=ref, send_sem=send_sem.at[0], recv_sem=sem,
            device_id={"sp": me}, device_id_type=MESH,
        ).wait_recv()

    def own(n):
        for kind in (OWN_Z, OWN_Y, OWN_C):
            start(kind, n)

    forwards = {4: (F4_Y, F4_C, F4_Z), 8: (F8_Y, F8_C), 2: (F2_C,), 6: (F6_C,)}

    def event(slot, n):
        @pl.when(me >= slot)
        def _():
            landed(chunk(n, slot), recv_sem.at[slot // 2, n])

        for kind in forwards[slot]:
            start(kind, n)
        if slot == 4 and 1 <= n < total - 2:
            own(n + 2)

    def near(kind, g, n):
        for slots in range(1, 5):
            first = 2 * slots - 1
            span = win.at[g, 0:slots] if kind == BOTH else win.at[g, 0:slots, kind]
            there = (me >= first) if slots == 4 else (me >= first) & (me < first + 2)

            @pl.when(there)
            def _():
                landed(span, recv_sem.at[0, n])

    value_copies = [
        pltpu.make_async_copy(
            v_hbm.at[:, pl.ds(g * HEAD_SIZE, HEAD_SIZE)],
            win.at[g, REACH, VALUE],
            value_sem.at[min(g, 1)],
        )
        for g in range(groups)
    ]
    small = [
        pltpu.make_async_copy(source, target, in_sem.at[i])
        for i, (source, target) in enumerate([
            (pos_hbm, pos_ref), (freq_hbm, freq_ref), (kg_hbm, kg_ref), (k_hbm, k_ref),
            (start_hbm, start_ref), (qg_hbm, qg_ref),
        ])
    ]
    width = copies * HEAD_SIZE
    query_copies = [
        pltpu.make_async_copy(
            q_hbm.at[:, pl.ds(i * HEAD_SIZE, HEAD_SIZE)], q_ref.at[i], query_sem.at[min(i // copies, 1)]
        )
        for i in range(groups * copies)
    ]
    barrier = pltpu.get_barrier_semaphore()
    for peer in (core_peer, side_peer):
        pl.semaphore_signal(barrier, inc=1, device_id={"sp": peer}, device_id_type=MESH)

    @pl.when(has_next)
    def _():
        pl.semaphore_signal(barrier, inc=1, device_id={"sp": me + 4}, device_id_type=MESH)

    @pl.when(me >= 4)
    def _():
        pl.semaphore_signal(barrier, inc=1, device_id={"sp": me - 4}, device_id_type=MESH)

    for copy in value_copies[:1] + small + value_copies[1:] + query_copies:
        copy.start()

    value_copies[0].wait()
    inner = (me >= 4) & has_next

    @pl.when(inner)
    def _():
        pl.semaphore_wait(barrier, 4)

    @pl.when(jnp.logical_not(inner))
    def _():
        pl.semaphore_wait(barrier, 3 if count > 4 else 2)

    own(0)
    for copy in small:
        copy.wait()
    places = jnp.broadcast_to(pos_ref[...].astype(jnp.float32), (HEAD_SIZE, rows)).T
    angle = places * freq_ref[...]
    lane = lax.broadcasted_iota(jnp.int32, (rows, HEAD_SIZE), 1)
    cos_full = jnp.cos(angle)
    sine = jnp.sin(angle)
    sin_full = jnp.where(lane < HEAD_SIZE // 2, -sine, sine)
    swap = (
        lax.rem(lax.broadcasted_iota(jnp.int32, (HEAD_SIZE, HEAD_SIZE), 0) + HEAD_SIZE // 2, HEAD_SIZE)
        == lax.broadcasted_iota(jnp.int32, (HEAD_SIZE, HEAD_SIZE), 1)
    ).astype(jnp.bfloat16)

    def tables(gain_ref):
        gain = jnp.broadcast_to(gain_ref[...], (rows, HEAD_SIZE))
        return gain * cos_full, pltpu.roll(gain, HEAD_SIZE // 2, axis=1) * sin_full

    straight, crossed = tables(kg_ref)
    for g in range(groups):
        rotated = norm_rope(k_ref[:, g * HEAD_SIZE:(g + 1) * HEAD_SIZE], swap, straight, crossed)
        win[g, REACH, KEY] = rotated.T.astype(jnp.bfloat16)
        if g == 0:
            rest = v_hbm.at[:, pl.ds(HEAD_SIZE, (groups - 1) * HEAD_SIZE)]
            pltpu.make_async_copy(rest, rest, value_sem.at[1]).wait()
            own(1)
    own(2)
    straight, crossed = tables(qg_ref)

    starts = jnp.broadcast_to(start_ref[...], (rows, rows)).T
    token = me * rows + lax.broadcasted_iota(jnp.int32, (rows, rows), 0)
    for b in range(REACH + 1):
        key_index = (me - REACH + b) * rows + lax.broadcasted_iota(jnp.int32, (rows, rows), 1)
        visible = (key_index >= starts) & (key_index <= token)
        hidden[b] = jnp.where(visible, 0.0, HIDDEN).astype(jnp.bfloat16)

    @pl.loop(0, jnp.maximum(REACH - me, 0))
    def _(j):
        for g in range(groups):
            win[g, j] = jnp.zeros((2, rows, HEAD_SIZE), jnp.bfloat16)

    weights_buf[tiles - 1][...] = jnp.zeros((blocks, tile_rows, rows), jnp.bfloat16)

    scale = HEAD_SIZE ** (-0.5) * math.log2(math.e)
    unit = (
        lax.broadcasted_iota(jnp.int32, (rows, rows), 0)
        == lax.broadcasted_iota(jnp.int32, (rows, rows), 1)
    ).astype(jnp.bfloat16)
    units = jnp.concatenate([unit] * Q_TILE, axis=0)

    def prepare(g):
        if g < 2:
            some = q_hbm.at[:, pl.ds(g * width, width if g == 0 else (groups - 1) * width)]
            pltpu.make_async_copy(some, some, query_sem.at[g]).wait()
        for head_index in range(copies):
            q_rope[g, head_index * rows:(head_index + 1) * rows] = norm_rope(
                q_ref[g * copies + head_index], swap, straight, crossed
            ).astype(jnp.bfloat16)

    def score(g, tile):
        queries = jnp.concatenate(
            [q_rope[g, tile * tile_rows:(tile + 1) * tile_rows], units], axis=1
        )
        best = None
        for b in range(0, blocks, 2):
            pair = range(b, min(b + 2, blocks))
            keys = jnp.concatenate([
                jnp.concatenate([win[g, i, KEY] for i in pair], axis=1),
                jnp.concatenate([hidden[i] for i in pair], axis=1),
            ], axis=0)
            part = jnp.dot(queries, keys, preferred_element_type=jnp.float32)
            for at, i in enumerate(pair):
                piece = part[:, at * rows:(at + 1) * rows]
                scores_buf[tile % 2][i] = piece
                best = piece if best is None else jnp.maximum(best, piece)
        top_buf[tile % 2][...] = best

    def soften(tile):
        top = jnp.max(top_buf[tile % 2][...], axis=1, keepdims=True)
        for b in range(blocks):
            part = scores_buf[tile % 2][b]
            weights_buf[tile][b] = jnp.exp2((part - top) * scale).astype(jnp.bfloat16)

    def mix(g, tile):
        values = jnp.concatenate([
            jnp.concatenate([win[g, b, VALUE] for b in range(blocks)], axis=0),
            jnp.ones((blocks * rows, HEAD_SIZE), jnp.bfloat16),
        ], axis=1)
        weights = jnp.concatenate([weights_buf[tile][b] for b in range(blocks)], axis=1)
        mixed = jnp.dot(weights, values, preferred_element_type=jnp.float32)
        mixed = mixed[:, :HEAD_SIZE] / mixed[:, HEAD_SIZE:]
        for r in range(Q_TILE):
            o_ref[g * copies + tile * Q_TILE + r] = mixed[r * rows:(r + 1) * rows].astype(jnp.bfloat16)

    arrivals = expected_arrivals([2 if kind == BOTH else 1 for kind, _ in order])
    first_tile = [when for when, slot, n in arrivals if (slot, n) == (6, 1)][0] + 0.1
    early = [(slot, n) for when, slot, n in arrivals if when < first_tile]
    by_block, tail = {}, []
    block = 2 * (groups - 1)
    for when, slot, n in reversed(arrivals):
        if when >= first_tile:
            at = max(int((when - first_tile - 1.5) / BLOCK_STEP), 0)
            block = min(block, at, max(2 * n - 3, 0) if n < total - 2 else at)
            if block < 2 * (groups - 1):
                by_block.setdefault(block, []).insert(0, (slot, n))
            else:
                tail.insert(0, (slot, n))

    ready = min(3, groups)
    for g in range(ready):
        prepare(g)
    for slot, n in early:
        event(slot, n)
        if ready < groups:
            prepare(ready)
            ready += 1
    for g in range(ready, groups):
        prepare(g)

    def relays(g, tile):
        for block, todo in by_block.items():
            if block % 2 != tile:
                continue
            if isinstance(g, int):
                if g == block // 2:
                    for slot, n in todo:
                        event(slot, n)
            elif block // 2 < groups - 2:
                @pl.when(g == block // 2)
                def _():
                    for slot, n in todo:
                        event(slot, n)

    near(VALUE, 0, 0)
    near(KEY, 0, 1)
    score(0, 0)

    last = groups - 1

    @pl.loop(0, last - 1)
    def _(g):
        relays(g, 0)
        score(g, 1)
        soften(0)
        mix(jnp.maximum(g - 1, 0), 1)
        relays(g, 1)
        near(BOTH, g + 1, g + 2)
        score(g + 1, 0)
        soften(1)
        mix(g, 0)

    relays(last - 1, 0)
    score(last - 1, 1)
    soften(0)
    mix(last - 2, 1)
    relays(last - 1, 1)
    soften(1)
    mix(last - 1, 0)
    for slot, n in tail:
        event(slot, n)
    mix(last - 1, 1)
    near(KEY, last, total - 2)
    for tile in range(tiles):
        score(last, tile)
    for tile in range(tiles):
        soften(tile)
    near(VALUE, last, total - 1)
    for tile in range(tiles):
        mix(last, tile)

    whole = win.at[:, REACH]
    for kind, (condition, _, _, target) in plan.items():
        @pl.when(condition)
        def _():
            pltpu.make_async_remote_copy(
                src_ref=whole, dst_ref=whole, send_sem=send_sem.at[kind],
                recv_sem=recv_sem.at[0, 0], device_id={"sp": target}, device_id_type=MESH,
            ).wait_send()


def leave(heads_ref, o_hbm, sem):
    for i in range(heads_ref.shape[0]):
        at = pl.ds(i * HEAD_SIZE, HEAD_SIZE)
        pltpu.make_async_copy(heads_ref.at[i], o_hbm.at[:, at], sem).start()
    pltpu.make_async_copy(o_hbm, o_hbm, sem).wait()


def solution(mesh):
    count = mesh.shape["sp"]

    def body(query_proj, key_projection, value_projection, query_gain, key_norm_gain, positions, doc_start):
        rows = query_proj.shape[0]
        groups = key_projection.shape[1] // HEAD_SIZE
        copies = query_proj.shape[1] // key_projection.shape[1]
        assert rows * REACH >= DOC_MAX and count % 4 == 0
        assert rows == HEAD_SIZE and groups >= 4 and copies == 2 * Q_TILE
        half_dim = HEAD_SIZE // 2
        inv_freq = ROPE_BASE ** (-(np.arange(half_dim) * 2.0 / HEAD_SIZE))
        freq = jnp.asarray(np.concatenate([inv_freq, inv_freq])[None, :], jnp.float32)
        blocks = REACH + 1
        tile_rows = Q_TILE * rows
        heads = pl.pallas_call(
            functools.partial(kernel, count, groups, copies, rows),
            out_shape=jax.ShapeDtypeStruct((groups * copies, rows, HEAD_SIZE), jnp.bfloat16),
            in_specs=[pl.BlockSpec(memory_space=pl.ANY)] * 8,
            out_specs=pl.BlockSpec(memory_space=pltpu.VMEM),
            scratch_shapes=[
                pltpu.VMEM((groups, blocks, 2, rows, HEAD_SIZE), jnp.bfloat16),
                pltpu.VMEM((blocks, rows, rows), jnp.bfloat16),
                pltpu.VMEM((groups * copies, rows, HEAD_SIZE), jnp.bfloat16),
                pltpu.VMEM(key_projection.shape, jnp.bfloat16),
                pltpu.VMEM((groups, copies * rows, HEAD_SIZE), jnp.bfloat16),
                pltpu.VMEM((blocks, tile_rows, rows), jnp.float32),
                pltpu.VMEM((blocks, tile_rows, rows), jnp.float32),
                pltpu.VMEM((tile_rows, rows), jnp.float32),
                pltpu.VMEM((tile_rows, rows), jnp.float32),
                pltpu.VMEM((blocks, tile_rows, rows), jnp.bfloat16),
                pltpu.VMEM((blocks, tile_rows, rows), jnp.bfloat16),
                pltpu.VMEM((1, HEAD_SIZE), jnp.float32),
                pltpu.VMEM((1, HEAD_SIZE), jnp.float32),
                pltpu.VMEM((1, HEAD_SIZE), jnp.float32),
                pltpu.VMEM((1, rows), jnp.int32),
                pltpu.VMEM((1, rows), jnp.int32),
                pltpu.SemaphoreType.DMA((2,)),
                pltpu.SemaphoreType.DMA((6,)),
                pltpu.SemaphoreType.DMA((2,)),
                pltpu.SemaphoreType.DMA((10,)),
                pltpu.SemaphoreType.DMA((5, groups + 2)),
            ],
            compiler_params=pltpu.CompilerParams(
                collective_id=0, has_side_effects=True, vmem_limit_bytes=41943040
            ),
        )(
            *(pltpu.with_memory_space_constraint(array, pltpu.HBM) for array in (
                query_proj, key_projection, value_projection,
                query_gain[None, :], key_norm_gain[None, :], freq, positions[None, :], doc_start[None, :],
            ))
        )
        return pl.pallas_call(
            leave,
            out_shape=jax.ShapeDtypeStruct(query_proj.shape, jnp.bfloat16),
            in_specs=[pl.BlockSpec(memory_space=pltpu.VMEM)],
            out_specs=pl.BlockSpec(memory_space=pl.ANY),
            scratch_shapes=[pltpu.SemaphoreType.DMA],
            compiler_params=pltpu.CompilerParams(vmem_limit_bytes=8 * 1024 * 1024),
        )(heads)

    tokens = P(("dp", "sp"), None)
    vector = P(("dp", "sp"))
    return jax.shard_map(
        body,
        mesh=mesh,
        in_specs=(tokens, tokens, tokens, P(), P(), vector, vector),
        out_specs=tokens,
        check_vma=False,
    )
```

```python
import functools
import math

import jax
import jax.numpy as jnp
import numpy as np
from jax import lax
from jax.experimental import pallas as pl
from jax.experimental.pallas import tpu as pltpu
from jax.sharding import PartitionSpec as P

HEAD_SIZE = 128
DOC_MAX = 1024
REACH = 8
ROPE_BASE = 1000000.0
NORM_EPS = 1e-06
HIDDEN = -1e30
Q_TILE = 1
AHEAD = 2
NEAR_TIME = 2.0
FAR_TIME = 1.5
CORE_HOP = 1.6
PATIENCE = 0.5
EARLIER = 1
MESH = pl.DeviceIdType.MESH

KEY, VALUE, BOTH = 0, 1, 2
OWN_Z, OWN_Y, OWN_C, F4_Z, F4_Y, F4_C, F8_Y, F8_C, F2_C, F6_C = range(10)
CHIP_KINDS = (OWN_Z, OWN_Y, F4_Z, F4_Y, F8_Y)


def norm_rope(block, swap, straight, crossed):
    up = block.astype(jnp.float32)
    mean_square = jnp.mean(up * up, axis=-1, keepdims=True)
    swapped = jnp.dot(block, swap, preferred_element_type=jnp.float32)
    return (up * straight + swapped * crossed) * lax.rsqrt(mean_square + NORM_EPS)


def chunk_order(groups):
    middle = [(BOTH, g) for g in range(1, groups - 1)]
    return [(VALUE, 0), (KEY, 0)] + middle + [(KEY, groups - 1), (VALUE, groups - 1)]


def expected_arrivals(sizes):
    total = len(sizes)
    line = [("own", n) for n in range(3)] + [("far", 0)]
    for n in range(1, total):
        line += [("far", n)] + ([("own", n + 2)] if n + 2 < total else [])
    at, end = 0.0, {}
    for item in line:
        at += sizes[item[1]]
        end[item] = at
    arrivals = []
    for n in range(total):
        arrivals += [(end["own", n] + 2.7, 4, n), (end["far", n] + 2.7, 8, n)]
    free = 0.0
    for when, slot, n in sorted(arrivals):
        free = max(free, when) + sizes[n]
        arrivals.append((free + 3.7, slot - 2, n))
    return sorted(arrivals)


def kernel(
    count, groups, copies, rows,
    q_hbm, k_hbm, v_hbm, qg_hbm, kg_hbm, freq_hbm, pos_hbm, start_hbm,
    o_ref, win, hidden, q_ref, k_ref, q_rope, sums, tops,
    qg_ref, kg_ref, freq_ref, pos_ref, start_ref,
    value_sem, in_sem, query_sem, send_sem, recv_sem,
):
    me = lax.axis_index("sp")
    core = lax.rem(me, 2)
    side = lax.rem(lax.div(me, 2), 2)
    core_peer = me + 1 - 2 * core
    side_peer = me + 2 - 4 * side
    blocks = REACH + 1
    tiles = copies // Q_TILE
    tile_rows = Q_TILE * rows

    order = chunk_order(groups)
    total = len(order)

    def chunk(n, slot):
        kind, g = order[n]
        if kind == BOTH:
            return win.at[g, REACH - slot]
        return win.at[g, REACH - slot, kind]

    def semaphore_of(kind, target_slot):
        if kind in CHIP_KINDS:
            return target_slot // 2
        return 0 if kind in (OWN_C, F2_C) else 5 if kind in (F6_C, F8_C) else (5 - 5 * core)

    def send(kind, n, source, target_slot, target):
        return pltpu.make_async_remote_copy(
            src_ref=chunk(n, source),
            dst_ref=chunk(n, target_slot),
            send_sem=send_sem.at[kind],
            recv_sem=recv_sem.at[semaphore_of(kind, target_slot), n],
            device_id={"sp": target},
            device_id_type=MESH,
        )

    has_next = me + 4 < count
    f4_slot = 6 - 4 * side

    plan = {
        OWN_Z: (has_next, 0, 4, me + 4),
        OWN_Y: (side == 0, 0, 2, side_peer),
        OWN_C: (core == 0, 0, 1, core_peer),
        F4_Z: ((me >= 4) & has_next, 4, 8, me + 4),
        F4_Y: (me >= 4, 4, f4_slot, side_peer),
        F4_C: (me >= 4, 4, 5 - 2 * core, core_peer),
        F8_Y: ((me >= 8) & (side == 1), 8, 6, side_peer),
        F8_C: ((me >= 8) & (core == 1), 8, 7, core_peer),
        F2_C: (me >= 2, 2, 3 - 2 * core, core_peer),
        F6_C: (me >= 6, 6, 7 - 2 * core, core_peer),
    }

    def start(kind, n):
        condition, source, target_slot, target = plan[kind]

        @pl.when(condition)
        def _():
            send(kind, n, source, target_slot, target).start()

    def landed(ref, sem):
        pltpu.make_async_remote_copy(
            src_ref=ref, dst_ref=ref, send_sem=send_sem.at[0], recv_sem=sem,
            device_id={"sp": me}, device_id_type=MESH,
        ).wait_recv()

    def own(n):
        for kind in (OWN_Z, OWN_Y, OWN_C):
            start(kind, n)

    forwards = {4: (F4_Y, F4_C, F4_Z), 8: (F8_Y, F8_C), 2: (F2_C,), 6: (F6_C,)}

    def event(slot, n):
        @pl.when(me >= slot)
        def _():
            landed(chunk(n, slot), recv_sem.at[slot // 2, n])

        for kind in forwards[slot]:
            start(kind, n)
        if slot == 4 and 1 <= n < total - 2:
            own(n + 2)

    def from_peer(far, kind, g, n):
        least, sem = (5, 5) if far else (1, 0)
        for slots, there in ((1, (me >= least) & (me < least + 2)), (2, me >= least + 2)):
            span = win.at[g, 0:slots] if kind == BOTH else win.at[g, 0:slots, kind]

            @pl.when(there)
            def _():
                landed(span, recv_sem.at[sem, n])

    value_copies = [
        pltpu.make_async_copy(
            v_hbm.at[:, pl.ds(g * HEAD_SIZE, HEAD_SIZE)],
            win.at[g, REACH, VALUE],
            value_sem.at[min(g, 1)],
        )
        for g in range(groups)
    ]
    small = [
        pltpu.make_async_copy(source, target, in_sem.at[i])
        for i, (source, target) in enumerate([
            (pos_hbm, pos_ref), (freq_hbm, freq_ref), (kg_hbm, kg_ref), (k_hbm, k_ref),
            (start_hbm, start_ref), (qg_hbm, qg_ref),
        ])
    ]
    width = copies * HEAD_SIZE
    query_copies = [
        pltpu.make_async_copy(
            q_hbm.at[:, pl.ds(i * HEAD_SIZE, HEAD_SIZE)], q_ref.at[i], query_sem.at[min(i // copies, 1)]
        )
        for i in range(groups * copies)
    ]
    barrier = pltpu.get_barrier_semaphore()
    for peer in (core_peer, side_peer):
        pl.semaphore_signal(barrier, inc=1, device_id={"sp": peer}, device_id_type=MESH)

    @pl.when(has_next)
    def _():
        pl.semaphore_signal(barrier, inc=1, device_id={"sp": me + 4}, device_id_type=MESH)

    @pl.when(me >= 4)
    def _():
        pl.semaphore_signal(barrier, inc=1, device_id={"sp": me - 4}, device_id_type=MESH)

    for copy in value_copies[:1] + small + value_copies[1:] + query_copies:
        copy.start()

    value_copies[0].wait()
    inner = (me >= 4) & has_next

    @pl.when(inner)
    def _():
        pl.semaphore_wait(barrier, 4)

    @pl.when(jnp.logical_not(inner))
    def _():
        pl.semaphore_wait(barrier, 3 if count > 4 else 2)

    own(0)
    for copy in small:
        copy.wait()
    places = jnp.broadcast_to(pos_ref[...].astype(jnp.float32), (HEAD_SIZE, rows)).T
    angle = places * freq_ref[...]
    lane = lax.broadcasted_iota(jnp.int32, (rows, HEAD_SIZE), 1)
    cos_full = jnp.cos(angle)
    sine = jnp.sin(angle)
    sin_full = jnp.where(lane < HEAD_SIZE // 2, -sine, sine)
    swap = (
        lax.rem(lax.broadcasted_iota(jnp.int32, (HEAD_SIZE, HEAD_SIZE), 0) + HEAD_SIZE // 2, HEAD_SIZE)
        == lax.broadcasted_iota(jnp.int32, (HEAD_SIZE, HEAD_SIZE), 1)
    ).astype(jnp.bfloat16)

    def tables(gain_ref):
        gain = jnp.broadcast_to(gain_ref[...], (rows, HEAD_SIZE))
        return gain * cos_full, pltpu.roll(gain, HEAD_SIZE // 2, axis=1) * sin_full

    straight, crossed = tables(kg_ref)
    for g in range(groups):
        rotated = norm_rope(k_ref[:, g * HEAD_SIZE:(g + 1) * HEAD_SIZE], swap, straight, crossed)
        win[g, REACH, KEY] = rotated.T.astype(jnp.bfloat16)
        if g == 0:
            rest = v_hbm.at[:, pl.ds(HEAD_SIZE, (groups - 1) * HEAD_SIZE)]
            pltpu.make_async_copy(rest, rest, value_sem.at[1]).wait()
            own(1)
    own(2)
    straight, crossed = tables(qg_ref)

    starts = jnp.broadcast_to(start_ref[...], (rows, rows)).T
    token = me * rows + lax.broadcasted_iota(jnp.int32, (rows, rows), 0)
    for b in range(REACH + 1):
        key_index = (me - REACH + b) * rows + lax.broadcasted_iota(jnp.int32, (rows, rows), 1)
        visible = (key_index >= starts) & (key_index <= token)
        hidden[b] = jnp.where(visible, 0.0, HIDDEN).astype(jnp.bfloat16)

    @pl.loop(0, jnp.maximum(REACH - me, 0))
    def _(j):
        for g in range(groups):
            win[g, j] = jnp.zeros((2, rows, HEAD_SIZE), jnp.bfloat16)

    scale = HEAD_SIZE ** (-0.5) * math.log2(math.e)
    unit = (
        lax.broadcasted_iota(jnp.int32, (rows, rows), 0)
        == lax.broadcasted_iota(jnp.int32, (rows, rows), 1)
    ).astype(jnp.bfloat16)
    units = jnp.concatenate([unit] * Q_TILE, axis=0)

    def prepare(g):
        if g < 2:
            some = q_hbm.at[:, pl.ds(g * width, width if g == 0 else (groups - 1) * width)]
            pltpu.make_async_copy(some, some, query_sem.at[g]).wait()
        for head_index in range(copies):
            q_rope[g, head_index * rows:(head_index + 1) * rows] = norm_rope(
                q_ref[g * copies + head_index], swap, straight, crossed
            ).astype(jnp.bfloat16)

    def operands(g, chosen):
        keys = jnp.concatenate([
            jnp.concatenate([win[g, b, KEY] for b in chosen], axis=1),
            jnp.concatenate([hidden[b] for b in chosen], axis=1),
        ], axis=0)
        values = jnp.concatenate([
            jnp.concatenate([win[g, b, VALUE] for b in chosen], axis=0),
            jnp.ones((len(chosen) * rows, HEAD_SIZE), jnp.bfloat16),
        ], axis=1)
        return keys, values

    def queries_of(g, tile):
        return jnp.concatenate([q_rope[g, tile * tile_rows:(tile + 1) * tile_rows], units], axis=1)

    far_blocks = range(0, REACH // 2)
    near_blocks = range(REACH // 2, blocks)

    def attend_near(g):
        keys, values = operands(g, near_blocks)
        for tile in range(tiles):
            scores = jnp.dot(queries_of(g, tile), keys, preferred_element_type=jnp.float32)
            top = jnp.max(scores, axis=1, keepdims=True)
            weights = jnp.exp2((scores - top) * scale).astype(jnp.bfloat16)
            sums[g, tile] = jnp.dot(weights, values, preferred_element_type=jnp.float32)
            tops[g, tile] = jnp.broadcast_to(top, (tile_rows, HEAD_SIZE))

    def attend_far(g):
        keys, values = operands(g, far_blocks)
        for tile in range(tiles):
            scores = jnp.dot(queries_of(g, tile), keys, preferred_element_type=jnp.float32)
            near_top = tops[g, tile]
            top = jnp.maximum(near_top, jnp.max(scores, axis=1, keepdims=True))
            wide = jnp.concatenate([top] * len(far_blocks), axis=1)
            weights = jnp.exp2((scores - wide) * scale).astype(jnp.bfloat16)
            factor = jnp.exp2((near_top - top) * scale)
            mixed = jnp.dot(weights, values, preferred_element_type=jnp.float32)
            mixed = sums[g, tile] * jnp.concatenate([factor, factor], axis=1) + mixed
            mixed = mixed[:, :HEAD_SIZE] / mixed[:, HEAD_SIZE:]
            for r in range(Q_TILE):
                o_ref[g * copies + tile * Q_TILE + r] = mixed[r * rows:(r + 1) * rows].astype(jnp.bfloat16)

    arrivals = expected_arrivals([2 if kind == BOTH else 1 for kind, _ in order])
    last = groups - 1
    plan_of_blocks = [("near", g) for g in range(AHEAD)]
    for g in range(groups):
        plan_of_blocks += [("far", g)] + ([("near", g + AHEAD)] if g + AHEAD < groups else [])
    pieces = [[n for n in range(total) if order[n][1] == g] for g in range(groups)]
    when_of = {(slot, n): when for when, slot, n in arrivals}
    clock, starts_at = 0.0, []
    for what, g in plan_of_blocks:
        slot = 6 if what == "far" else 2
        clock = max([clock] + [when_of[slot, n] + CORE_HOP for n in pieces[g]])
        starts_at.append(clock)
        clock += FAR_TIME if what == "far" else NEAR_TIME
    reader = {(what, g): i for i, (what, g) in enumerate(plan_of_blocks)}
    by_block = {}
    block = len(plan_of_blocks) - 1
    for when, slot, n in reversed(arrivals):
        at = [i for i, begin in enumerate(starts_at) if begin > when - PATIENCE]
        read = reader["far" if slot in (6, 8) else "near", order[n][1]]
        block = min([block, max(read - EARLIER, 0) if read < len(plan_of_blocks) - 1 else read] + at[:1])
        by_block.setdefault(block, []).insert(0, (slot, n))
    early = by_block.pop(0)

    ready = min(3, groups)
    for g in range(ready):
        prepare(g)
    for slot, n in early:
        event(slot, n)
        if ready < groups:
            prepare(ready)
            ready += 1
    for g in range(ready, groups):
        prepare(g)

    def relays(block):
        for slot, n in by_block.get(block, []):
            event(slot, n)

    def relays_in_loop(g, first):
        for at in range(groups - AHEAD):
            if first + 2 * at in by_block:
                @pl.when(g == at)
                def _():
                    relays(first + 2 * at)

    def await_pieces(far, g):
        for n in pieces[g]:
            from_peer(far, order[n][0], g, n)

    for g in range(AHEAD):
        if g:
            relays(g)
        await_pieces(False, g)
        attend_near(g)

    @pl.loop(0, groups - AHEAD)
    def _(g):
        relays_in_loop(g, AHEAD)

        @pl.when(g == 0)
        def _():
            await_pieces(True, 0)

        @pl.when(g > 0)
        def _():
            from_peer(True, BOTH, jnp.maximum(g, 1), jnp.maximum(g, 1) + 1)

        attend_far(g)
        relays_in_loop(g, AHEAD + 1)

        @pl.when(g + AHEAD < last)
        def _():
            other = jnp.minimum(g + AHEAD, last - 1)
            from_peer(False, BOTH, other, other + 1)

        @pl.when(g + AHEAD == last)
        def _():
            await_pieces(False, last)

        attend_near(g + AHEAD)

    for g in range(groups - AHEAD, groups):
        relays(reader["far", g])
        await_pieces(True, g)
        attend_far(g)

    whole = win.at[:, REACH]
    for kind, (condition, _, _, target) in plan.items():
        @pl.when(condition)
        def _():
            pltpu.make_async_remote_copy(
                src_ref=whole, dst_ref=whole, send_sem=send_sem.at[kind],
                recv_sem=recv_sem.at[0, 0], device_id={"sp": target}, device_id_type=MESH,
            ).wait_send()


def leave(heads_ref, o_hbm, sem):
    for i in range(heads_ref.shape[0]):
        at = pl.ds(i * HEAD_SIZE, HEAD_SIZE)
        pltpu.make_async_copy(heads_ref.at[i], o_hbm.at[:, at], sem).start()
    pltpu.make_async_copy(o_hbm, o_hbm, sem).wait()


def solution(mesh):
    count = mesh.shape["sp"]

    def body(query_proj, key_projection, value_projection, query_gain, key_norm_gain, positions, doc_start):
        rows = query_proj.shape[0]
        groups = key_projection.shape[1] // HEAD_SIZE
        copies = query_proj.shape[1] // key_projection.shape[1]
        assert rows * REACH >= DOC_MAX and count % 4 == 0
        assert rows == HEAD_SIZE and groups >= 4 and copies % Q_TILE == 0
        half_dim = HEAD_SIZE // 2
        inv_freq = ROPE_BASE ** (-(np.arange(half_dim) * 2.0 / HEAD_SIZE))
        freq = jnp.asarray(np.concatenate([inv_freq, inv_freq])[None, :], jnp.float32)
        blocks = REACH + 1
        heads = pl.pallas_call(
            functools.partial(kernel, count, groups, copies, rows),
            out_shape=jax.ShapeDtypeStruct((groups * copies, rows, HEAD_SIZE), jnp.bfloat16),
            in_specs=[pl.BlockSpec(memory_space=pl.ANY)] * 8,
            out_specs=pl.BlockSpec(memory_space=pltpu.VMEM),
            scratch_shapes=[
                pltpu.VMEM((groups, blocks, 2, rows, HEAD_SIZE), jnp.bfloat16),
                pltpu.VMEM((blocks, rows, rows), jnp.bfloat16),
                pltpu.VMEM((groups * copies, rows, HEAD_SIZE), jnp.bfloat16),
                pltpu.VMEM(key_projection.shape, jnp.bfloat16),
                pltpu.VMEM((groups, copies * rows, HEAD_SIZE), jnp.bfloat16),
                pltpu.VMEM((groups, copies // Q_TILE, Q_TILE * rows, 2 * HEAD_SIZE), jnp.float32),
                pltpu.VMEM((groups, copies // Q_TILE, Q_TILE * rows, HEAD_SIZE), jnp.float32),
                pltpu.VMEM((1, HEAD_SIZE), jnp.float32),
                pltpu.VMEM((1, HEAD_SIZE), jnp.float32),
                pltpu.VMEM((1, HEAD_SIZE), jnp.float32),
                pltpu.VMEM((1, rows), jnp.int32),
                pltpu.VMEM((1, rows), jnp.int32),
                pltpu.SemaphoreType.DMA((2,)),
                pltpu.SemaphoreType.DMA((6,)),
                pltpu.SemaphoreType.DMA((2,)),
                pltpu.SemaphoreType.DMA((10,)),
                pltpu.SemaphoreType.DMA((6, groups + 2)),
            ],
            compiler_params=pltpu.CompilerParams(
                collective_id=0, has_side_effects=True, vmem_limit_bytes=41943040
            ),
        )(
            *(pltpu.with_memory_space_constraint(array, pltpu.HBM) for array in (
                query_proj, key_projection, value_projection,
                query_gain[None, :], key_norm_gain[None, :], freq, positions[None, :], doc_start[None, :],
            ))
        )
        return pl.pallas_call(
            leave,
            out_shape=jax.ShapeDtypeStruct(query_proj.shape, jnp.bfloat16),
            in_specs=[pl.BlockSpec(memory_space=pltpu.VMEM)],
            out_specs=pl.BlockSpec(memory_space=pl.ANY),
            scratch_shapes=[pltpu.SemaphoreType.DMA],
            compiler_params=pltpu.CompilerParams(vmem_limit_bytes=8 * 1024 * 1024),
        )(heads)

    tokens = P(("dp", "sp"), None)
    vector = P(("dp", "sp"))
    return jax.shard_map(
        body,
        mesh=mesh,
        in_specs=(tokens, tokens, tokens, P(), P(), vector, vector),
        out_specs=tokens,
        check_vma=False,
    )
```

```python
import functools
import math

import jax
import jax.numpy as jnp
import numpy as np
from jax import lax
from jax.experimental import pallas as pl
from jax.experimental.pallas import tpu as pltpu
from jax.sharding import PartitionSpec as P

HEAD_SIZE = 128
DOC_MAX = 1024
REACH = 8
ROPE_BASE = 1000000.0
NORM_EPS = 1e-06
HIDDEN = -1e30
Q_TILE = 1
AHEAD = 2
NEAR_TIME = 2.0
FAR_TIME = 1.5
CORE_HOP = 1.6
PATIENCE = 0.5
EARLIER = 1
MESH = pl.DeviceIdType.MESH

KEY, VALUE, BOTH = 0, 1, 2
OWN_Z, OWN_Y, OWN_C, F4_Z, F4_Y, F4_C, F8_Y, F8_C, F2_C, F6_C = range(10)
CHIP_KINDS = (OWN_Z, OWN_Y, F4_Z, F4_Y, F8_Y)


def norm_rope(block, swap, straight, crossed):
    up = block.astype(jnp.float32)
    mean_square = jnp.mean(up * up, axis=-1, keepdims=True)
    swapped = jnp.dot(block, swap, preferred_element_type=jnp.float32)
    return (up * straight + swapped * crossed) * lax.rsqrt(mean_square + NORM_EPS)


def chunk_order(groups):
    middle = [(BOTH, g) for g in range(1, groups - 1)]
    return [(VALUE, 0), (KEY, 0)] + middle + [(KEY, groups - 1), (VALUE, groups - 1)]


def released(total, n):
    if n < 1 or n > total - 4:
        return []
    if n == total - 4:
        return [total - 1]
    return [n + 2] if n < total - 5 else [n + 2, n + 3]


def expected_arrivals(sizes):
    total = len(sizes)
    line = [("own", n) for n in range(3)] + [("far", 0)]
    for n in range(1, total):
        line += [("far", n)] + [("own", m) for m in released(total, n)]
    at, end = 0.0, {}
    for item in line:
        at += sizes[item[1]]
        end[item] = at
    arrivals = []
    for n in range(total):
        arrivals += [(end["own", n] + 2.7, 4, n), (end["far", n] + 2.7, 8, n)]
    free = 0.0
    for when, slot, n in sorted(arrivals):
        free = max(free, when) + sizes[n]
        arrivals.append((free + 3.7, slot - 2, n))
    return sorted(arrivals)


def kernel(
    count, groups, copies, rows,
    q_hbm, k_hbm, v_hbm, qg_hbm, kg_hbm, freq_hbm, pos_hbm, start_hbm,
    o_ref, win, hidden, q_ref, k_ref, q_rope, sums, tops,
    qg_ref, kg_ref, freq_ref, pos_ref, start_ref,
    value_sem, in_sem, query_sem, send_sem, recv_sem,
):
    me = lax.axis_index("sp")
    core = lax.rem(me, 2)
    side = lax.rem(lax.div(me, 2), 2)
    core_peer = me + 1 - 2 * core
    side_peer = me + 2 - 4 * side
    blocks = REACH + 1
    tiles = copies // Q_TILE
    tile_rows = Q_TILE * rows

    order = chunk_order(groups)
    total = len(order)

    def chunk(n, slot):
        kind, g = order[n]
        if kind == BOTH:
            return win.at[g, REACH - slot]
        return win.at[g, REACH - slot, kind]

    def semaphore_of(kind, target_slot):
        if kind in CHIP_KINDS:
            return target_slot // 2
        return 0 if kind in (OWN_C, F2_C) else 5 if kind in (F6_C, F8_C) else (5 - 5 * core)

    def send(kind, n, source, target_slot, target):
        return pltpu.make_async_remote_copy(
            src_ref=chunk(n, source),
            dst_ref=chunk(n, target_slot),
            send_sem=send_sem.at[kind],
            recv_sem=recv_sem.at[semaphore_of(kind, target_slot), n],
            device_id={"sp": target},
            device_id_type=MESH,
        )

    has_next = me + 4 < count
    f4_slot = 6 - 4 * side

    plan = {
        OWN_Z: (has_next, 0, 4, me + 4),
        OWN_Y: (side == 0, 0, 2, side_peer),
        OWN_C: (core == 0, 0, 1, core_peer),
        F4_Z: ((me >= 4) & has_next, 4, 8, me + 4),
        F4_Y: (me >= 4, 4, f4_slot, side_peer),
        F4_C: (me >= 4, 4, 5 - 2 * core, core_peer),
        F8_Y: ((me >= 8) & (side == 1), 8, 6, side_peer),
        F8_C: ((me >= 8) & (core == 1), 8, 7, core_peer),
        F2_C: (me >= 2, 2, 3 - 2 * core, core_peer),
        F6_C: (me >= 6, 6, 7 - 2 * core, core_peer),
    }

    def start(kind, n):
        condition, source, target_slot, target = plan[kind]

        @pl.when(condition)
        def _():
            send(kind, n, source, target_slot, target).start()

    def landed(ref, sem):
        pltpu.make_async_remote_copy(
            src_ref=ref, dst_ref=ref, send_sem=send_sem.at[0], recv_sem=sem,
            device_id={"sp": me}, device_id_type=MESH,
        ).wait_recv()

    def own(n):
        for kind in (OWN_Z, OWN_Y, OWN_C):
            start(kind, n)

    forwards = {4: (F4_Y, F4_C, F4_Z), 8: (F8_Y, F8_C), 2: (F2_C,), 6: (F6_C,)}

    def event(slot, n):
        @pl.when(me >= slot)
        def _():
            landed(chunk(n, slot), recv_sem.at[slot // 2, n])

        for kind in forwards[slot]:
            start(kind, n)
        for m in released(total, n) if slot == 4 else ():
            own(m)

    def from_peer(far, kind, g, n):
        least, sem = (5, 5) if far else (1, 0)
        for slots, there in ((1, (me >= least) & (me < least + 2)), (2, me >= least + 2)):
            span = win.at[g, 0:slots] if kind == BOTH else win.at[g, 0:slots, kind]

            @pl.when(there)
            def _():
                landed(span, recv_sem.at[sem, n])

    value_copies = [
        pltpu.make_async_copy(
            v_hbm.at[:, pl.ds(g * HEAD_SIZE, HEAD_SIZE)],
            win.at[g, REACH, VALUE],
            value_sem.at[min(g, 1)],
        )
        for g in range(groups)
    ]
    small = [
        pltpu.make_async_copy(source, target, in_sem.at[i])
        for i, (source, target) in enumerate([
            (pos_hbm, pos_ref), (freq_hbm, freq_ref), (kg_hbm, kg_ref), (k_hbm, k_ref),
            (start_hbm, start_ref), (qg_hbm, qg_ref),
        ])
    ]
    width = copies * HEAD_SIZE
    query_copies = [
        pltpu.make_async_copy(
            q_hbm.at[:, pl.ds(i * HEAD_SIZE, HEAD_SIZE)], q_ref.at[i], query_sem.at[min(i // copies, 1)]
        )
        for i in range(groups * copies)
    ]
    barrier = pltpu.get_barrier_semaphore()
    for peer in (core_peer, side_peer):
        pl.semaphore_signal(barrier, inc=1, device_id={"sp": peer}, device_id_type=MESH)

    @pl.when(has_next)
    def _():
        pl.semaphore_signal(barrier, inc=1, device_id={"sp": me + 4}, device_id_type=MESH)

    @pl.when(me >= 4)
    def _():
        pl.semaphore_signal(barrier, inc=1, device_id={"sp": me - 4}, device_id_type=MESH)

    for copy in value_copies[:1] + small + value_copies[1:]:
        copy.start()

    value_copies[0].wait()
    inner = (me >= 4) & has_next

    @pl.when(inner)
    def _():
        pl.semaphore_wait(barrier, 4)

    @pl.when(jnp.logical_not(inner))
    def _():
        pl.semaphore_wait(barrier, 3 if count > 4 else 2)

    own(0)
    for copy in query_copies:
        copy.start()
    for copy in small:
        copy.wait()
    places = jnp.broadcast_to(pos_ref[...].astype(jnp.float32), (HEAD_SIZE, rows)).T
    angle = places * freq_ref[...]
    lane = lax.broadcasted_iota(jnp.int32, (rows, HEAD_SIZE), 1)
    cos_full = jnp.cos(angle)
    sine = jnp.sin(angle)
    sin_full = jnp.where(lane < HEAD_SIZE // 2, -sine, sine)
    swap = (
        lax.rem(lax.broadcasted_iota(jnp.int32, (HEAD_SIZE, HEAD_SIZE), 0) + HEAD_SIZE // 2, HEAD_SIZE)
        == lax.broadcasted_iota(jnp.int32, (HEAD_SIZE, HEAD_SIZE), 1)
    ).astype(jnp.bfloat16)

    def tables(gain_ref):
        gain = jnp.broadcast_to(gain_ref[...], (rows, HEAD_SIZE))
        return gain * cos_full, pltpu.roll(gain, HEAD_SIZE // 2, axis=1) * sin_full

    straight, crossed = tables(kg_ref)
    for g in range(groups):
        rotated = norm_rope(k_ref[:, g * HEAD_SIZE:(g + 1) * HEAD_SIZE], swap, straight, crossed)
        win[g, REACH, KEY] = rotated.T.astype(jnp.bfloat16)
        if g == 0:
            rest = v_hbm.at[:, pl.ds(HEAD_SIZE, (groups - 1) * HEAD_SIZE)]
            pltpu.make_async_copy(rest, rest, value_sem.at[1]).wait()
            own(1)
    own(2)
    straight, crossed = tables(qg_ref)

    starts = jnp.broadcast_to(start_ref[...], (rows, rows)).T
    token = me * rows + lax.broadcasted_iota(jnp.int32, (rows, rows), 0)
    for b in range(REACH + 1):
        key_index = (me - REACH + b) * rows + lax.broadcasted_iota(jnp.int32, (rows, rows), 1)
        visible = (key_index >= starts) & (key_index <= token)
        hidden[b] = jnp.where(visible, 0.0, HIDDEN).astype(jnp.bfloat16)

    @pl.loop(0, jnp.maximum(REACH - me, 0))
    def _(j):
        for g in range(groups):
            win[g, j] = jnp.zeros((2, rows, HEAD_SIZE), jnp.bfloat16)

    scale = HEAD_SIZE ** (-0.5) * math.log2(math.e)
    unit = (
        lax.broadcasted_iota(jnp.int32, (rows, rows), 0)
        == lax.broadcasted_iota(jnp.int32, (rows, rows), 1)
    ).astype(jnp.bfloat16)
    units = jnp.concatenate([unit] * Q_TILE, axis=0)

    def prepare(g):
        if g < 2:
            some = q_hbm.at[:, pl.ds(g * width, width if g == 0 else (groups - 1) * width)]
            pltpu.make_async_copy(some, some, query_sem.at[g]).wait()
        for head_index in range(copies):
            q_rope[g, head_index * rows:(head_index + 1) * rows] = norm_rope(
                q_ref[g * copies + head_index], swap, straight, crossed
            ).astype(jnp.bfloat16)

    def operands(g, chosen):
        keys = jnp.concatenate([
            jnp.concatenate([win[g, b, KEY] for b in chosen], axis=1),
            jnp.concatenate([hidden[b] for b in chosen], axis=1),
        ], axis=0)
        values = jnp.concatenate([
            jnp.concatenate([win[g, b, VALUE] for b in chosen], axis=0),
            jnp.ones((len(chosen) * rows, HEAD_SIZE), jnp.bfloat16),
        ], axis=1)
        return keys, values

    def queries_of(g, tile):
        return jnp.concatenate([q_rope[g, tile * tile_rows:(tile + 1) * tile_rows], units], axis=1)

    far_blocks = range(0, REACH // 2)
    near_blocks = range(REACH // 2, blocks)

    def attend_near(g):
        keys, values = operands(g, near_blocks)
        for tile in range(tiles):
            scores = jnp.dot(queries_of(g, tile), keys, preferred_element_type=jnp.float32)
            top = jnp.max(scores, axis=1, keepdims=True)
            weights = jnp.exp2((scores - top) * scale).astype(jnp.bfloat16)
            sums[g, tile] = jnp.dot(weights, values, preferred_element_type=jnp.float32)
            tops[g, tile] = jnp.broadcast_to(top, (tile_rows, HEAD_SIZE))

    def attend_far(g):
        keys, values = operands(g, far_blocks)
        for tile in range(tiles):
            scores = jnp.dot(queries_of(g, tile), keys, preferred_element_type=jnp.float32)
            near_top = tops[g, tile]
            top = jnp.maximum(near_top, jnp.max(scores, axis=1, keepdims=True))
            wide = jnp.concatenate([top] * len(far_blocks), axis=1)
            weights = jnp.exp2((scores - wide) * scale).astype(jnp.bfloat16)
            factor = jnp.exp2((near_top - top) * scale)
            mixed = jnp.dot(weights, values, preferred_element_type=jnp.float32)
            mixed = sums[g, tile] * jnp.concatenate([factor, factor], axis=1) + mixed
            mixed = mixed[:, :HEAD_SIZE] / mixed[:, HEAD_SIZE:]
            for r in range(Q_TILE):
                o_ref[g * copies + tile * Q_TILE + r] = mixed[r * rows:(r + 1) * rows].astype(jnp.bfloat16)

    arrivals = expected_arrivals([2 if kind == BOTH else 1 for kind, _ in order])
    last = groups - 1
    plan_of_blocks = [("near", g) for g in range(AHEAD)]
    for g in range(groups):
        plan_of_blocks += [("far", g)] + ([("near", g + AHEAD)] if g + AHEAD < groups else [])
    pieces = [[n for n in range(total) if order[n][1] == g] for g in range(groups)]
    when_of = {(slot, n): when for when, slot, n in arrivals}
    clock, starts_at = 0.0, []
    for what, g in plan_of_blocks:
        slot = 6 if what == "far" else 2
        clock = max([clock] + [when_of[slot, n] + CORE_HOP for n in pieces[g]])
        starts_at.append(clock)
        clock += FAR_TIME if what == "far" else NEAR_TIME
    reader = {(what, g): i for i, (what, g) in enumerate(plan_of_blocks)}
    by_block = {}
    block = len(plan_of_blocks) - 1
    for when, slot, n in reversed(arrivals):
        at = [i for i, begin in enumerate(starts_at) if begin > when - PATIENCE]
        read = reader["far" if slot in (6, 8) else "near", order[n][1]]
        block = min([block, max(read - EARLIER, 0) if read < len(plan_of_blocks) - 1 else read] + at[:1])
        by_block.setdefault(block, []).insert(0, (slot, n))
    early = by_block.pop(0)

    ready = min(3, groups)
    for g in range(ready):
        prepare(g)
    for slot, n in early:
        event(slot, n)
        if ready < groups:
            prepare(ready)
            ready += 1
    for g in range(ready, groups):
        prepare(g)

    def relays(block):
        for slot, n in by_block.get(block, []):
            event(slot, n)

    def relays_in_loop(g, first):
        for at in range(groups - AHEAD):
            if first + 2 * at in by_block:
                @pl.when(g == at)
                def _():
                    relays(first + 2 * at)

    def await_pieces(far, g):
        for n in pieces[g]:
            from_peer(far, order[n][0], g, n)

    for g in range(AHEAD):
        if g:
            relays(g)
        await_pieces(False, g)
        attend_near(g)

    @pl.loop(0, groups - AHEAD)
    def _(g):
        relays_in_loop(g, AHEAD)

        @pl.when(g == 0)
        def _():
            await_pieces(True, 0)

        @pl.when(g > 0)
        def _():
            from_peer(True, BOTH, jnp.maximum(g, 1), jnp.maximum(g, 1) + 1)

        attend_far(g)
        relays_in_loop(g, AHEAD + 1)

        @pl.when(g + AHEAD < last)
        def _():
            other = jnp.minimum(g + AHEAD, last - 1)
            from_peer(False, BOTH, other, other + 1)

        @pl.when(g + AHEAD == last)
        def _():
            await_pieces(False, last)

        attend_near(g + AHEAD)

    for g in range(groups - AHEAD, groups):
        relays(reader["far", g])
        await_pieces(True, g)
        attend_far(g)

    whole = win.at[:, REACH]
    for kind, (condition, _, _, target) in plan.items():
        @pl.when(condition)
        def _():
            pltpu.make_async_remote_copy(
                src_ref=whole, dst_ref=whole, send_sem=send_sem.at[kind],
                recv_sem=recv_sem.at[0, 0], device_id={"sp": target}, device_id_type=MESH,
            ).wait_send()


def leave(heads_ref, o_hbm, sem):
    for i in range(heads_ref.shape[0]):
        at = pl.ds(i * HEAD_SIZE, HEAD_SIZE)
        pltpu.make_async_copy(heads_ref.at[i], o_hbm.at[:, at], sem).start()
    pltpu.make_async_copy(o_hbm, o_hbm, sem).wait()


def solution(mesh):
    count = mesh.shape["sp"]

    def body(query_proj, key_projection, value_projection, query_gain, key_norm_gain, positions, doc_start):
        rows = query_proj.shape[0]
        groups = key_projection.shape[1] // HEAD_SIZE
        copies = query_proj.shape[1] // key_projection.shape[1]
        assert rows * REACH >= DOC_MAX and count % 4 == 0
        assert rows == HEAD_SIZE and groups >= 6 and copies % Q_TILE == 0
        half_dim = HEAD_SIZE // 2
        inv_freq = ROPE_BASE ** (-(np.arange(half_dim) * 2.0 / HEAD_SIZE))
        freq = jnp.asarray(np.concatenate([inv_freq, inv_freq])[None, :], jnp.float32)
        blocks = REACH + 1
        heads = pl.pallas_call(
            functools.partial(kernel, count, groups, copies, rows),
            out_shape=jax.ShapeDtypeStruct((groups * copies, rows, HEAD_SIZE), jnp.bfloat16),
            in_specs=[pl.BlockSpec(memory_space=pl.ANY)] * 8,
            out_specs=pl.BlockSpec(memory_space=pltpu.VMEM),
            scratch_shapes=[
                pltpu.VMEM((groups, blocks, 2, rows, HEAD_SIZE), jnp.bfloat16),
                pltpu.VMEM((blocks, rows, rows), jnp.bfloat16),
                pltpu.VMEM((groups * copies, rows, HEAD_SIZE), jnp.bfloat16),
                pltpu.VMEM(key_projection.shape, jnp.bfloat16),
                pltpu.VMEM((groups, copies * rows, HEAD_SIZE), jnp.bfloat16),
                pltpu.VMEM((groups, copies // Q_TILE, Q_TILE * rows, 2 * HEAD_SIZE), jnp.float32),
                pltpu.VMEM((groups, copies // Q_TILE, Q_TILE * rows, HEAD_SIZE), jnp.float32),
                pltpu.VMEM((1, HEAD_SIZE), jnp.float32),
                pltpu.VMEM((1, HEAD_SIZE), jnp.float32),
                pltpu.VMEM((1, HEAD_SIZE), jnp.float32),
                pltpu.VMEM((1, rows), jnp.int32),
                pltpu.VMEM((1, rows), jnp.int32),
                pltpu.SemaphoreType.DMA((2,)),
                pltpu.SemaphoreType.DMA((6,)),
                pltpu.SemaphoreType.DMA((2,)),
                pltpu.SemaphoreType.DMA((10,)),
                pltpu.SemaphoreType.DMA((6, groups + 2)),
            ],
            compiler_params=pltpu.CompilerParams(
                collective_id=0, has_side_effects=True, vmem_limit_bytes=41943040
            ),
        )(
            *(pltpu.with_memory_space_constraint(array, pltpu.HBM) for array in (
                query_proj, key_projection, value_projection,
                query_gain[None, :], key_norm_gain[None, :], freq, positions[None, :], doc_start[None, :],
            ))
        )
        return pl.pallas_call(
            leave,
            out_shape=jax.ShapeDtypeStruct(query_proj.shape, jnp.bfloat16),
            in_specs=[pl.BlockSpec(memory_space=pltpu.VMEM)],
            out_specs=pl.BlockSpec(memory_space=pl.ANY),
            scratch_shapes=[pltpu.SemaphoreType.DMA],
            compiler_params=pltpu.CompilerParams(vmem_limit_bytes=8 * 1024 * 1024),
        )(heads)

    tokens = P(("dp", "sp"), None)
    vector = P(("dp", "sp"))
    return jax.shard_map(
        body,
        mesh=mesh,
        in_specs=(tokens, tokens, tokens, P(), P(), vector, vector),
        out_specs=tokens,
        check_vma=False,
    )
```

```python
import functools
import math

import jax
import jax.numpy as jnp
import numpy as np
from jax import lax
from jax.experimental import pallas as pl
from jax.experimental.pallas import tpu as pltpu
from jax.sharding import PartitionSpec as P

HEAD_SIZE = 128
DOC_MAX = 1024
REACH = 8
ROPE_BASE = 1000000.0
NORM_EPS = 1e-06
HIDDEN = -1e30
Q_TILE = 1
AHEAD = 2
NEAR_TIME = 2.0
FAR_TIME = 1.5
CORE_HOP = 1.6
PATIENCE = 0.5
EARLIER = 1
MESH = pl.DeviceIdType.MESH

KEY, VALUE, BOTH = 0, 1, 2
OWN_Z, OWN_Y, OWN_C, F4_Z, F4_Y, F4_C, F8_Y, F8_C, F2_C, F6_C = range(10)
CHIP_KINDS = (OWN_Z, OWN_Y, F4_Z, F4_Y, F8_Y)


def norm_rope(block, swap, straight, crossed):
    up = block.astype(jnp.float32)
    mean_square = jnp.mean(up * up, axis=-1, keepdims=True)
    swapped = jnp.dot(block, swap, preferred_element_type=jnp.float32)
    return (up * straight + swapped * crossed) * lax.rsqrt(mean_square + NORM_EPS)


def chunk_order(groups):
    middle = [(BOTH, g) for g in range(1, groups - 1)]
    return [(VALUE, 0), (KEY, 0)] + middle + [(KEY, groups - 1), (VALUE, groups - 1)]


def released(total, n):
    if n < 1 or n > total - 4:
        return []
    if n == total - 4:
        return [total - 1]
    return [n + 2] if n < total - 5 else [n + 2, n + 3]


def expected_arrivals(sizes):
    total = len(sizes)
    line = [("own", n) for n in range(3)] + [("far", 0)]
    for n in range(1, total):
        line += [("far", n)] + [("own", m) for m in released(total, n)]
    at, end = 0.0, {}
    for item in line:
        at += sizes[item[1]]
        end[item] = at
    arrivals = []
    for n in range(total):
        arrivals += [(end["own", n] + 2.7, 4, n), (end["far", n] + 2.7, 8, n)]
    free = 0.0
    for when, slot, n in sorted(arrivals):
        free = max(free, when) + sizes[n]
        arrivals.append((free + 3.7, slot - 2, n))
    return sorted(arrivals)


SCALE = HEAD_SIZE ** (-0.5) * math.log2(math.e)


def unit_rows(rows):
    unit = (
        lax.broadcasted_iota(jnp.int32, (rows, rows), 0)
        == lax.broadcasted_iota(jnp.int32, (rows, rows), 1)
    ).astype(jnp.bfloat16)
    return jnp.concatenate([unit] * Q_TILE, axis=0)


def operands(win, hidden, g, chosen):
    rows = win.shape[3]
    keys = jnp.concatenate([
        jnp.concatenate([win[g, b, KEY] for b in chosen], axis=1),
        jnp.concatenate([hidden[b] for b in chosen], axis=1),
    ], axis=0)
    values = jnp.concatenate([
        jnp.concatenate([win[g, b, VALUE] for b in chosen], axis=0),
        jnp.ones((len(chosen) * rows, HEAD_SIZE), jnp.bfloat16),
    ], axis=1)
    return keys, values


def queries_of(q_rope, units, g, tile):
    size = units.shape[0]
    return jnp.concatenate([q_rope[g, tile * size:(tile + 1) * size], units], axis=1)


def attend_near(win, hidden, q_rope, sums, tops, units, g):
    keys, values = operands(win, hidden, g, range(REACH // 2, REACH + 1))
    for tile in range(sums.shape[1]):
        scores = jnp.dot(queries_of(q_rope, units, g, tile), keys, preferred_element_type=jnp.float32)
        top = jnp.max(scores, axis=1, keepdims=True)
        weights = jnp.exp2((scores - top) * SCALE).astype(jnp.bfloat16)
        sums[g, tile] = jnp.dot(weights, values, preferred_element_type=jnp.float32)
        tops[g, tile] = jnp.broadcast_to(top, tops.shape[2:])


def attend_far(win, hidden, q_rope, sums, tops, units, g, o_ref, first):
    rows = win.shape[3]
    keys, values = operands(win, hidden, g, range(REACH // 2))
    for tile in range(sums.shape[1]):
        scores = jnp.dot(queries_of(q_rope, units, g, tile), keys, preferred_element_type=jnp.float32)
        near_top = tops[g, tile]
        top = jnp.maximum(near_top, jnp.max(scores, axis=1, keepdims=True))
        wide = jnp.concatenate([top] * (REACH // 2), axis=1)
        weights = jnp.exp2((scores - wide) * SCALE).astype(jnp.bfloat16)
        factor = jnp.exp2((near_top - top) * SCALE)
        mixed = jnp.dot(weights, values, preferred_element_type=jnp.float32)
        mixed = sums[g, tile] * jnp.concatenate([factor, factor], axis=1) + mixed
        mixed = mixed[:, :HEAD_SIZE] / mixed[:, HEAD_SIZE:]
        for r in range(Q_TILE):
            o_ref[first + tile * Q_TILE + r] = mixed[r * rows:(r + 1) * rows].astype(jnp.bfloat16)


def kernel(
    count, groups, copies, rows,
    q_hbm, k_hbm, v_hbm, qg_hbm, kg_hbm, freq_hbm, pos_hbm, start_hbm,
    o_ref, win, hidden, q_rope, sums, tops, q_ref, k_ref,
    qg_ref, kg_ref, freq_ref, pos_ref, start_ref,
    value_sem, in_sem, query_sem, send_sem, recv_sem,
):
    me = lax.axis_index("sp")
    core = lax.rem(me, 2)
    side = lax.rem(lax.div(me, 2), 2)
    core_peer = me + 1 - 2 * core
    side_peer = me + 2 - 4 * side
    blocks = REACH + 1

    order = chunk_order(groups)
    total = len(order)

    def chunk(n, slot):
        kind, g = order[n]
        if kind == BOTH:
            return win.at[g, REACH - slot]
        return win.at[g, REACH - slot, kind]

    def semaphore_of(kind, target_slot):
        if kind in CHIP_KINDS:
            return target_slot // 2
        return 0 if kind in (OWN_C, F2_C) else 5 if kind in (F6_C, F8_C) else (5 - 5 * core)

    def send(kind, n, source, target_slot, target):
        return pltpu.make_async_remote_copy(
            src_ref=chunk(n, source),
            dst_ref=chunk(n, target_slot),
            send_sem=send_sem.at[kind],
            recv_sem=recv_sem.at[semaphore_of(kind, target_slot), n],
            device_id={"sp": target},
            device_id_type=MESH,
        )

    has_next = me + 4 < count
    f4_slot = 6 - 4 * side

    plan = {
        OWN_Z: (has_next, 0, 4, me + 4),
        OWN_Y: (side == 0, 0, 2, side_peer),
        OWN_C: (core == 0, 0, 1, core_peer),
        F4_Z: ((me >= 4) & has_next, 4, 8, me + 4),
        F4_Y: (me >= 4, 4, f4_slot, side_peer),
        F4_C: (me >= 4, 4, 5 - 2 * core, core_peer),
        F8_Y: ((me >= 8) & (side == 1), 8, 6, side_peer),
        F8_C: ((me >= 8) & (core == 1), 8, 7, core_peer),
        F2_C: (me >= 2, 2, 3 - 2 * core, core_peer),
        F6_C: (me >= 6, 6, 7 - 2 * core, core_peer),
    }

    def start(kind, n):
        condition, source, target_slot, target = plan[kind]

        @pl.when(condition)
        def _():
            send(kind, n, source, target_slot, target).start()

    def landed(ref, sem):
        pltpu.make_async_remote_copy(
            src_ref=ref, dst_ref=ref, send_sem=send_sem.at[0], recv_sem=sem,
            device_id={"sp": me}, device_id_type=MESH,
        ).wait_recv()

    def own(n):
        for kind in (OWN_Z, OWN_Y, OWN_C):
            start(kind, n)

    forwards = {4: (F4_Y, F4_C, F4_Z), 8: (F8_Y, F8_C), 2: (F2_C,), 6: (F6_C,)}

    def event(slot, n):
        @pl.when(me >= slot)
        def _():
            landed(chunk(n, slot), recv_sem.at[slot // 2, n])

        for kind in forwards[slot]:
            start(kind, n)
        for m in released(total, n) if slot == 4 else ():
            own(m)

    def from_peer(far, kind, g, n):
        least, sem = (5, 5) if far else (1, 0)
        for slots, there in ((1, (me >= least) & (me < least + 2)), (2, me >= least + 2)):
            span = win.at[g, 0:slots] if kind == BOTH else win.at[g, 0:slots, kind]

            @pl.when(there)
            def _():
                landed(span, recv_sem.at[sem, n])

    value_copies = [
        pltpu.make_async_copy(
            v_hbm.at[:, pl.ds(g * HEAD_SIZE, HEAD_SIZE)],
            win.at[g, REACH, VALUE],
            value_sem.at[min(g, 1)],
        )
        for g in range(groups)
    ]
    small = [
        pltpu.make_async_copy(source, target, in_sem.at[i])
        for i, (source, target) in enumerate([
            (pos_hbm, pos_ref), (freq_hbm, freq_ref), (kg_hbm, kg_ref), (k_hbm, k_ref),
            (start_hbm, start_ref), (qg_hbm, qg_ref),
        ])
    ]
    width = copies * HEAD_SIZE
    query_copies = [
        pltpu.make_async_copy(
            q_hbm.at[:, pl.ds(i * HEAD_SIZE, HEAD_SIZE)], q_ref.at[i], query_sem.at[min(i // copies, 1)]
        )
        for i in range(groups * copies)
    ]
    barrier = pltpu.get_barrier_semaphore()
    for peer in (core_peer, side_peer):
        pl.semaphore_signal(barrier, inc=1, device_id={"sp": peer}, device_id_type=MESH)

    @pl.when(has_next)
    def _():
        pl.semaphore_signal(barrier, inc=1, device_id={"sp": me + 4}, device_id_type=MESH)

    @pl.when(me >= 4)
    def _():
        pl.semaphore_signal(barrier, inc=1, device_id={"sp": me - 4}, device_id_type=MESH)

    for copy in value_copies[:1] + small + value_copies[1:]:
        copy.start()

    value_copies[0].wait()
    inner = (me >= 4) & has_next

    @pl.when(inner)
    def _():
        pl.semaphore_wait(barrier, 4)

    @pl.when(jnp.logical_not(inner))
    def _():
        pl.semaphore_wait(barrier, 3 if count > 4 else 2)

    own(0)
    for copy in query_copies:
        copy.start()
    for copy in small:
        copy.wait()
    places = jnp.broadcast_to(pos_ref[...].astype(jnp.float32), (HEAD_SIZE, rows)).T
    angle = places * freq_ref[...]
    lane = lax.broadcasted_iota(jnp.int32, (rows, HEAD_SIZE), 1)
    cos_full = jnp.cos(angle)
    sine = jnp.sin(angle)
    sin_full = jnp.where(lane < HEAD_SIZE // 2, -sine, sine)
    swap = (
        lax.rem(lax.broadcasted_iota(jnp.int32, (HEAD_SIZE, HEAD_SIZE), 0) + HEAD_SIZE // 2, HEAD_SIZE)
        == lax.broadcasted_iota(jnp.int32, (HEAD_SIZE, HEAD_SIZE), 1)
    ).astype(jnp.bfloat16)

    def tables(gain_ref):
        gain = jnp.broadcast_to(gain_ref[...], (rows, HEAD_SIZE))
        return gain * cos_full, pltpu.roll(gain, HEAD_SIZE // 2, axis=1) * sin_full

    straight, crossed = tables(kg_ref)
    for g in range(groups):
        rotated = norm_rope(k_ref[:, g * HEAD_SIZE:(g + 1) * HEAD_SIZE], swap, straight, crossed)
        win[g, REACH, KEY] = rotated.T.astype(jnp.bfloat16)
        if g == 0:
            rest = v_hbm.at[:, pl.ds(HEAD_SIZE, (groups - 1) * HEAD_SIZE)]
            pltpu.make_async_copy(rest, rest, value_sem.at[1]).wait()
            own(1)
    own(2)
    straight, crossed = tables(qg_ref)

    starts = jnp.broadcast_to(start_ref[...], (rows, rows)).T
    token = me * rows + lax.broadcasted_iota(jnp.int32, (rows, rows), 0)
    for b in range(REACH + 1):
        key_index = (me - REACH + b) * rows + lax.broadcasted_iota(jnp.int32, (rows, rows), 1)
        visible = (key_index >= starts) & (key_index <= token)
        hidden[b] = jnp.where(visible, 0.0, HIDDEN).astype(jnp.bfloat16)

    @pl.loop(0, jnp.maximum(REACH - me, 0))
    def _(j):
        for g in range(groups):
            win[g, j] = jnp.zeros((2, rows, HEAD_SIZE), jnp.bfloat16)

    units = unit_rows(rows)

    def prepare(g):
        if g < 2:
            some = q_hbm.at[:, pl.ds(g * width, width if g == 0 else (groups - 1) * width)]
            pltpu.make_async_copy(some, some, query_sem.at[g]).wait()
        for head_index in range(copies):
            q_rope[g, head_index * rows:(head_index + 1) * rows] = norm_rope(
                q_ref[g * copies + head_index], swap, straight, crossed
            ).astype(jnp.bfloat16)

    def near(g):
        attend_near(win, hidden, q_rope, sums, tops, units, g)

    def far(g):
        attend_far(win, hidden, q_rope, sums, tops, units, g, o_ref, g * copies)

    arrivals = expected_arrivals([2 if kind == BOTH else 1 for kind, _ in order])
    last = groups - 1
    plan_of_blocks = [("near", g) for g in range(AHEAD)]
    for g in range(groups):
        plan_of_blocks += [("far", g)] + ([("near", g + AHEAD)] if g + AHEAD < groups else [])
    pieces = [[n for n in range(total) if order[n][1] == g] for g in range(groups)]
    when_of = {(slot, n): when for when, slot, n in arrivals}
    clock, starts_at = 0.0, []
    for what, g in plan_of_blocks:
        slot = 6 if what == "far" else 2
        clock = max([clock] + [when_of[slot, n] + CORE_HOP for n in pieces[g]])
        starts_at.append(clock)
        clock += FAR_TIME if what == "far" else NEAR_TIME
    reader = {(what, g): i for i, (what, g) in enumerate(plan_of_blocks)}
    by_block = {}
    block = len(plan_of_blocks) - 1
    for when, slot, n in reversed(arrivals):
        at = [i for i, begin in enumerate(starts_at) if begin > when - PATIENCE]
        read = reader["far" if slot in (6, 8) else "near", order[n][1]]
        block = min([block, max(read - EARLIER, 0) if read < len(plan_of_blocks) - 1 else read] + at[:1])
        by_block.setdefault(block, []).insert(0, (slot, n))
    early = by_block.pop(0)

    ready = min(3, groups)
    for g in range(ready):
        prepare(g)
    for slot, n in early:
        event(slot, n)
        if ready < groups:
            prepare(ready)
            ready += 1
    for g in range(ready, groups):
        prepare(g)

    def relays(block):
        for slot, n in by_block.get(block, []):
            event(slot, n)

    def relays_in_loop(g, first):
        for at in range(groups - AHEAD):
            if first + 2 * at in by_block:
                @pl.when(g == at)
                def _():
                    relays(first + 2 * at)

    def await_pieces(far, g):
        for n in pieces[g]:
            from_peer(far, order[n][0], g, n)

    for g in range(AHEAD):
        if g:
            relays(g)
        await_pieces(False, g)
        near(g)

    @pl.loop(0, groups - AHEAD)
    def _(g):
        relays_in_loop(g, AHEAD)

        @pl.when(g == 0)
        def _():
            await_pieces(True, 0)

        @pl.when(g > 0)
        def _():
            from_peer(True, BOTH, jnp.maximum(g, 1), jnp.maximum(g, 1) + 1)

        far(g)
        relays_in_loop(g, AHEAD + 1)

        @pl.when(g + AHEAD < last)
        def _():
            other = jnp.minimum(g + AHEAD, last - 1)
            from_peer(False, BOTH, other, other + 1)

        @pl.when(g + AHEAD == last)
        def _():
            await_pieces(False, last)

        near(g + AHEAD)

    for g in range(groups - AHEAD, groups):
        relays(reader["far", g])
        await_pieces(True, g)
        if g < last:
            far(g)

    whole = win.at[:, REACH]
    for kind, (condition, _, _, target) in plan.items():
        @pl.when(condition)
        def _():
            pltpu.make_async_remote_copy(
                src_ref=whole, dst_ref=whole, send_sem=send_sem.at[kind],
                recv_sem=recv_sem.at[0, 0], device_id={"sp": target}, device_id_type=MESH,
            ).wait_send()


def leave(heads, win, hidden, q_rope, sums, tops, o_hbm, last_heads, sem):
    done = heads.shape[0]

    def put(source, i):
        at = pl.ds(i * HEAD_SIZE, HEAD_SIZE)
        pltpu.make_async_copy(source, o_hbm.at[:, at], sem).start()

    for i in range(done):
        put(heads.at[i], i)
    units = unit_rows(win.shape[3])
    attend_far(win, hidden, q_rope, sums, tops, units, win.shape[0] - 1, last_heads, 0)
    for i in range(last_heads.shape[0]):
        put(last_heads.at[i], done + i)
    pltpu.make_async_copy(o_hbm, o_hbm, sem).wait()


def solution(mesh):
    count = mesh.shape["sp"]

    def body(query_proj, key_projection, value_projection, query_gain, key_norm_gain, positions, doc_start):
        rows = query_proj.shape[0]
        groups = key_projection.shape[1] // HEAD_SIZE
        copies = query_proj.shape[1] // key_projection.shape[1]
        assert rows * REACH >= DOC_MAX and count % 4 == 0
        assert rows == HEAD_SIZE and groups >= 6 and copies % Q_TILE == 0
        half_dim = HEAD_SIZE // 2
        inv_freq = ROPE_BASE ** (-(np.arange(half_dim) * 2.0 / HEAD_SIZE))
        freq = jnp.asarray(np.concatenate([inv_freq, inv_freq])[None, :], jnp.float32)
        blocks = REACH + 1
        tiles, tile_rows = copies // Q_TILE, Q_TILE * rows
        held = [
            jax.ShapeDtypeStruct(((groups - 1) * copies, rows, HEAD_SIZE), jnp.bfloat16),
            jax.ShapeDtypeStruct((groups, blocks, 2, rows, HEAD_SIZE), jnp.bfloat16),
            jax.ShapeDtypeStruct((blocks, rows, rows), jnp.bfloat16),
            jax.ShapeDtypeStruct((groups, copies * rows, HEAD_SIZE), jnp.bfloat16),
            jax.ShapeDtypeStruct((groups, tiles, tile_rows, 2 * HEAD_SIZE), jnp.float32),
            jax.ShapeDtypeStruct((groups, tiles, tile_rows, HEAD_SIZE), jnp.float32),
        ]
        state = pl.pallas_call(
            functools.partial(kernel, count, groups, copies, rows),
            out_shape=held,
            in_specs=[pl.BlockSpec(memory_space=pl.ANY)] * 8,
            out_specs=[pl.BlockSpec(memory_space=pltpu.VMEM)] * len(held),
            scratch_shapes=[
                pltpu.VMEM((groups * copies, rows, HEAD_SIZE), jnp.bfloat16),
                pltpu.VMEM(key_projection.shape, jnp.bfloat16),
                pltpu.VMEM((1, HEAD_SIZE), jnp.float32),
                pltpu.VMEM((1, HEAD_SIZE), jnp.float32),
                pltpu.VMEM((1, HEAD_SIZE), jnp.float32),
                pltpu.VMEM((1, rows), jnp.int32),
                pltpu.VMEM((1, rows), jnp.int32),
                pltpu.SemaphoreType.DMA((2,)),
                pltpu.SemaphoreType.DMA((6,)),
                pltpu.SemaphoreType.DMA((2,)),
                pltpu.SemaphoreType.DMA((10,)),
                pltpu.SemaphoreType.DMA((6, groups + 2)),
            ],
            compiler_params=pltpu.CompilerParams(
                collective_id=0, has_side_effects=True, vmem_limit_bytes=12 * 1024 * 1024
            ),
        )(
            *(pltpu.with_memory_space_constraint(array, pltpu.HBM) for array in (
                query_proj, key_projection, value_projection,
                query_gain[None, :], key_norm_gain[None, :], freq, positions[None, :], doc_start[None, :],
            ))
        )
        return pl.pallas_call(
            leave,
            out_shape=jax.ShapeDtypeStruct(query_proj.shape, jnp.bfloat16),
            in_specs=[pl.BlockSpec(memory_space=pltpu.VMEM)] * len(held),
            out_specs=pl.BlockSpec(memory_space=pl.ANY),
            scratch_shapes=[
                pltpu.VMEM((copies, rows, HEAD_SIZE), jnp.bfloat16), pltpu.SemaphoreType.DMA,
            ],
            compiler_params=pltpu.CompilerParams(vmem_limit_bytes=8 * 1024 * 1024),
        )(*state)

    tokens = P(("dp", "sp"), None)
    vector = P(("dp", "sp"))
    return jax.shard_map(
        body,
        mesh=mesh,
        in_specs=(tokens, tokens, tokens, P(), P(), vector, vector),
        out_specs=tokens,
        check_vma=False,
    )
```

```python
import functools
import math

import jax
import jax.numpy as jnp
import numpy as np
from jax import lax
from jax.experimental import pallas as pl
from jax.experimental.pallas import tpu as pltpu
from jax.sharding import PartitionSpec as P

HEAD_SIZE = 128
DOC_MAX = 1024
REACH = 8
ROPE_BASE = 1000000.0
NORM_EPS = 1e-06
HIDDEN = -1e30
Q_TILE = 1
AHEAD = 2
NEAR_TIME = 1.8
FAR_TIME = 1.5
CORE_HOP = 1.4
PATIENCE = 0.5
EARLIER = 1
MESH = pl.DeviceIdType.MESH

KEY, VALUE, BOTH = 0, 1, 2
OWN_Z, OWN_Y, OWN_C, F4_Z, F4_Y, F4_C, F8_Y, F8_C, F2_C, F6_C = range(10)
CHIP_KINDS = (OWN_Z, OWN_Y, F4_Z, F4_Y, F8_Y)


def norm_rope(block, swap, straight, crossed):
    up = block.astype(jnp.float32)
    mean_square = jnp.mean(up * up, axis=-1, keepdims=True)
    swapped = jnp.dot(block, swap, preferred_element_type=jnp.float32)
    return (up * straight + swapped * crossed) * lax.rsqrt(mean_square + NORM_EPS)


def chunk_order(groups):
    middle = [(BOTH, g) for g in range(1, groups - 1)]
    return [(VALUE, 0), (KEY, 0)] + middle + [(KEY, groups - 1), (VALUE, groups - 1)]


def released(total, n):
    if n < 1 or n > total - 4:
        return []
    if n == total - 4:
        return [total - 1]
    return [n + 2] if n < total - 5 else [n + 2, n + 3]


def expected_arrivals(sizes):
    total = len(sizes)
    line = [("own", n) for n in range(3)] + [("far", 0)]
    for n in range(1, total):
        line += [("far", n)] + [("own", m) for m in released(total, n)]
    at, end = 0.0, {}
    for item in line:
        at += sizes[item[1]]
        end[item] = at
    arrivals = []
    for n in range(total):
        arrivals += [(end["own", n] + 2.7, 4, n), (end["far", n] + 2.7, 8, n)]
    free = 0.0
    for when, slot, n in sorted(arrivals):
        free = max(free, when) + sizes[n]
        arrivals.append((free + 3.7, slot - 2, n))
    return sorted(arrivals)


SCALE = HEAD_SIZE ** (-0.5) * math.log2(math.e)


def unit_rows(rows):
    unit = (
        lax.broadcasted_iota(jnp.int32, (rows, rows), 0)
        == lax.broadcasted_iota(jnp.int32, (rows, rows), 1)
    ).astype(jnp.bfloat16)
    return jnp.concatenate([unit] * Q_TILE, axis=0)


def operands(win, hidden, g, chosen):
    rows = win.shape[3]
    keys = jnp.concatenate([
        jnp.concatenate([win[g, b, KEY] for b in chosen], axis=1),
        jnp.concatenate([hidden[b] for b in chosen], axis=1),
    ], axis=0)
    values = jnp.concatenate([
        jnp.concatenate([win[g, b, VALUE] for b in chosen], axis=0),
        jnp.ones((len(chosen) * rows, HEAD_SIZE), jnp.bfloat16),
    ], axis=1)
    return keys, values


def queries_of(q_rope, units, g, tile):
    size = units.shape[0]
    return jnp.concatenate([q_rope[g, tile * size:(tile + 1) * size], units], axis=1)


def attend_near(win, hidden, q_rope, sums, tops, units, g):
    keys, values = operands(win, hidden, g, range(REACH // 2, REACH + 1))
    for tile in range(sums.shape[1]):
        scores = jnp.dot(queries_of(q_rope, units, g, tile), keys, preferred_element_type=jnp.float32)
        top = jnp.max(scores, axis=1, keepdims=True)
        weights = jnp.exp2((scores - top) * SCALE).astype(jnp.bfloat16)
        sums[g, tile] = jnp.dot(weights, values, preferred_element_type=jnp.float32)
        tops[g, tile] = jnp.broadcast_to(top, tops.shape[2:])


def attend_far(win, hidden, q_rope, sums, tops, units, g, o_ref, first):
    rows = win.shape[3]
    keys, values = operands(win, hidden, g, range(REACH // 2))
    for tile in range(sums.shape[1]):
        scores = jnp.dot(queries_of(q_rope, units, g, tile), keys, preferred_element_type=jnp.float32)
        near_top = tops[g, tile]
        top = jnp.maximum(near_top, jnp.max(scores, axis=1, keepdims=True))
        wide = jnp.concatenate([top] * (REACH // 2), axis=1)
        weights = jnp.exp2((scores - wide) * SCALE).astype(jnp.bfloat16)
        factor = jnp.exp2((near_top - top) * SCALE)
        mixed = jnp.dot(weights, values, preferred_element_type=jnp.float32)
        mixed = sums[g, tile] * jnp.concatenate([factor, factor], axis=1) + mixed
        mixed = mixed[:, :HEAD_SIZE] / mixed[:, HEAD_SIZE:]
        for r in range(Q_TILE):
            o_ref[first + tile * Q_TILE + r] = mixed[r * rows:(r + 1) * rows].astype(jnp.bfloat16)


def kernel(
    count, groups, copies, rows,
    q_hbm, k_hbm, v_hbm, qg_hbm, kg_hbm, freq_hbm, pos_hbm, start_hbm,
    o_ref, win, hidden, q_rope, sums, tops, q_ref, k_ref,
    qg_ref, kg_ref, freq_ref, pos_ref, start_ref,
    value_sem, in_sem, query_sem, send_sem, recv_sem,
):
    me = lax.axis_index("sp")
    core = lax.rem(me, 2)
    side = lax.rem(lax.div(me, 2), 2)
    core_peer = me + 1 - 2 * core
    side_peer = me + 2 - 4 * side
    blocks = REACH + 1

    order = chunk_order(groups)
    total = len(order)

    def chunk(n, slot):
        kind, g = order[n]
        if kind == BOTH:
            return win.at[g, REACH - slot]
        return win.at[g, REACH - slot, kind]

    def semaphore_of(kind, target_slot):
        if kind in CHIP_KINDS:
            return target_slot // 2
        return 0 if kind in (OWN_C, F2_C) else 5 if kind in (F6_C, F8_C) else (5 - 5 * core)

    def send(kind, n, source, target_slot, target):
        return pltpu.make_async_remote_copy(
            src_ref=chunk(n, source),
            dst_ref=chunk(n, target_slot),
            send_sem=send_sem.at[kind],
            recv_sem=recv_sem.at[semaphore_of(kind, target_slot), n],
            device_id={"sp": target},
            device_id_type=MESH,
        )

    has_next = me + 4 < count
    f4_slot = 6 - 4 * side

    plan = {
        OWN_Z: (has_next, 0, 4, me + 4),
        OWN_Y: (side == 0, 0, 2, side_peer),
        OWN_C: (core == 0, 0, 1, core_peer),
        F4_Z: ((me >= 4) & has_next, 4, 8, me + 4),
        F4_Y: (me >= 4, 4, f4_slot, side_peer),
        F4_C: (me >= 4, 4, 5 - 2 * core, core_peer),
        F8_Y: ((me >= 8) & (side == 1), 8, 6, side_peer),
        F8_C: ((me >= 8) & (core == 1), 8, 7, core_peer),
        F2_C: (me >= 2, 2, 3 - 2 * core, core_peer),
        F6_C: (me >= 6, 6, 7 - 2 * core, core_peer),
    }

    def start(kind, n):
        condition, source, target_slot, target = plan[kind]

        @pl.when(condition)
        def _():
            send(kind, n, source, target_slot, target).start()

    def landed(ref, sem):
        pltpu.make_async_remote_copy(
            src_ref=ref, dst_ref=ref, send_sem=send_sem.at[0], recv_sem=sem,
            device_id={"sp": me}, device_id_type=MESH,
        ).wait_recv()

    def own(n):
        for kind in (OWN_Z, OWN_Y, OWN_C):
            start(kind, n)

    forwards = {4: (F4_C, F4_Z, F4_Y), 8: (F8_Y, F8_C), 2: (F2_C,), 6: (F6_C,)}

    def event(slot, n):
        @pl.when(me >= slot)
        def _():
            landed(chunk(n, slot), recv_sem.at[slot // 2, n])

        for kind in forwards[slot]:
            start(kind, n)
        for m in released(total, n) if slot == 4 else ():
            own(m)

    def from_peer(far, kind, g, n):
        least, sem = (5, 5) if far else (1, 0)
        for slots, there in ((1, (me >= least) & (me < least + 2)), (2, me >= least + 2)):
            span = win.at[g, 0:slots] if kind == BOTH else win.at[g, 0:slots, kind]

            @pl.when(there)
            def _():
                landed(span, recv_sem.at[sem, n])

    value_copies = [
        pltpu.make_async_copy(
            v_hbm.at[:, pl.ds(g * HEAD_SIZE, HEAD_SIZE)],
            win.at[g, REACH, VALUE],
            value_sem.at[min(g, 1)],
        )
        for g in range(groups)
    ]
    small = [
        pltpu.make_async_copy(source, target, in_sem.at[i])
        for i, (source, target) in enumerate([
            (pos_hbm, pos_ref), (freq_hbm, freq_ref), (kg_hbm, kg_ref), (k_hbm, k_ref),
            (start_hbm, start_ref), (qg_hbm, qg_ref),
        ])
    ]
    width = copies * HEAD_SIZE
    query_copies = [
        pltpu.make_async_copy(
            q_hbm.at[:, pl.ds(i * HEAD_SIZE, HEAD_SIZE)], q_ref.at[i], query_sem.at[min(i // copies, 1)]
        )
        for i in range(groups * copies)
    ]
    barrier = pltpu.get_barrier_semaphore()
    for peer in (core_peer, side_peer):
        pl.semaphore_signal(barrier, inc=1, device_id={"sp": peer}, device_id_type=MESH)

    @pl.when(has_next)
    def _():
        pl.semaphore_signal(barrier, inc=1, device_id={"sp": me + 4}, device_id_type=MESH)

    @pl.when(me >= 4)
    def _():
        pl.semaphore_signal(barrier, inc=1, device_id={"sp": me - 4}, device_id_type=MESH)

    for copy in value_copies[:1] + small + value_copies[1:]:
        copy.start()

    value_copies[0].wait()
    inner = (me >= 4) & has_next

    @pl.when(inner)
    def _():
        pl.semaphore_wait(barrier, 4)

    @pl.when(jnp.logical_not(inner))
    def _():
        pl.semaphore_wait(barrier, 3 if count > 4 else 2)

    own(0)
    for copy in query_copies:
        copy.start()
    for copy in small:
        copy.wait()
    places = jnp.broadcast_to(pos_ref[...].astype(jnp.float32), (HEAD_SIZE, rows)).T
    angle = places * freq_ref[...]
    lane = lax.broadcasted_iota(jnp.int32, (rows, HEAD_SIZE), 1)
    cos_full = jnp.cos(angle)
    sine = jnp.sin(angle)
    sin_full = jnp.where(lane < HEAD_SIZE // 2, -sine, sine)
    swap = (
        lax.rem(lax.broadcasted_iota(jnp.int32, (HEAD_SIZE, HEAD_SIZE), 0) + HEAD_SIZE // 2, HEAD_SIZE)
        == lax.broadcasted_iota(jnp.int32, (HEAD_SIZE, HEAD_SIZE), 1)
    ).astype(jnp.bfloat16)

    def tables(gain_ref):
        gain = jnp.broadcast_to(gain_ref[...], (rows, HEAD_SIZE))
        return gain * cos_full, pltpu.roll(gain, HEAD_SIZE // 2, axis=1) * sin_full

    straight, crossed = tables(kg_ref)
    for g in range(groups):
        rotated = norm_rope(k_ref[:, g * HEAD_SIZE:(g + 1) * HEAD_SIZE], swap, straight, crossed)
        win[g, REACH, KEY] = rotated.T.astype(jnp.bfloat16)
        if g == 0:
            rest = v_hbm.at[:, pl.ds(HEAD_SIZE, (groups - 1) * HEAD_SIZE)]
            pltpu.make_async_copy(rest, rest, value_sem.at[1]).wait()
            own(1)
    own(2)
    straight, crossed = tables(qg_ref)

    starts = jnp.broadcast_to(start_ref[...], (rows, rows)).T
    token = me * rows + lax.broadcasted_iota(jnp.int32, (rows, rows), 0)
    for b in range(REACH + 1):
        key_index = (me - REACH + b) * rows + lax.broadcasted_iota(jnp.int32, (rows, rows), 1)
        visible = (key_index >= starts) & (key_index <= token)
        hidden[b] = jnp.where(visible, 0.0, HIDDEN).astype(jnp.bfloat16)

    @pl.loop(0, jnp.maximum(REACH - me, 0))
    def _(j):
        for g in range(groups):
            win[g, j] = jnp.zeros((2, rows, HEAD_SIZE), jnp.bfloat16)

    units = unit_rows(rows)

    def prepare(g):
        if g < 2:
            some = q_hbm.at[:, pl.ds(g * width, width if g == 0 else (groups - 1) * width)]
            pltpu.make_async_copy(some, some, query_sem.at[g]).wait()
        for head_index in range(copies):
            q_rope[g, head_index * rows:(head_index + 1) * rows] = norm_rope(
                q_ref[g * copies + head_index], swap, straight, crossed
            ).astype(jnp.bfloat16)

    def near(g):
        attend_near(win, hidden, q_rope, sums, tops, units, g)

    def far(g):
        attend_far(win, hidden, q_rope, sums, tops, units, g, o_ref, g * copies)

    arrivals = expected_arrivals([2 if kind == BOTH else 1 for kind, _ in order])
    last = groups - 1
    plan_of_blocks = [("near", g) for g in range(AHEAD)]
    for g in range(groups):
        plan_of_blocks += [("far", g)] + ([("near", g + AHEAD)] if g + AHEAD < groups else [])
    pieces = [[n for n in range(total) if order[n][1] == g] for g in range(groups)]
    when_of = {(slot, n): when for when, slot, n in arrivals}
    clock, starts_at = 0.0, []
    for what, g in plan_of_blocks:
        slot = 6 if what == "far" else 2
        clock = max([clock] + [when_of[slot, n] + CORE_HOP for n in pieces[g]])
        starts_at.append(clock)
        clock += FAR_TIME if what == "far" else NEAR_TIME
    reader = {(what, g): i for i, (what, g) in enumerate(plan_of_blocks)}
    by_block = {}
    block = len(plan_of_blocks) - 1
    for when, slot, n in reversed(arrivals):
        at = [i for i, begin in enumerate(starts_at) if begin > when - PATIENCE]
        read = reader["far" if slot in (6, 8) else "near", order[n][1]]
        block = min([block, max(read - EARLIER, 0) if read < len(plan_of_blocks) - 1 else read] + at[:1])
        by_block.setdefault(block, []).insert(0, (slot, n))
    early = by_block.pop(0)

    ready = min(3, groups)
    for g in range(ready):
        prepare(g)
    for slot, n in early:
        event(slot, n)
        if ready < groups:
            prepare(ready)
            ready += 1
    for g in range(ready, groups):
        prepare(g)

    def relays(block):
        for slot, n in by_block.get(block, []):
            event(slot, n)

    def relays_in_loop(g, first):
        for at in range(groups - AHEAD):
            if first + 2 * at in by_block:
                @pl.when(g == at)
                def _():
                    relays(first + 2 * at)

    def await_pieces(far, g):
        for n in pieces[g]:
            from_peer(far, order[n][0], g, n)

    for g in range(AHEAD):
        if g:
            relays(g)
        await_pieces(False, g)
        near(g)

    @pl.loop(0, groups - AHEAD)
    def _(g):
        relays_in_loop(g, AHEAD)

        @pl.when(g == 0)
        def _():
            await_pieces(True, 0)

        @pl.when(g > 0)
        def _():
            from_peer(True, BOTH, jnp.maximum(g, 1), jnp.maximum(g, 1) + 1)

        far(g)
        relays_in_loop(g, AHEAD + 1)

        @pl.when(g + AHEAD < last)
        def _():
            other = jnp.minimum(g + AHEAD, last - 1)
            from_peer(False, BOTH, other, other + 1)

        @pl.when(g + AHEAD == last)
        def _():
            await_pieces(False, last)

        near(g + AHEAD)

    for g in range(groups - AHEAD, groups):
        relays(reader["far", g])
        await_pieces(True, g)
        if g < last:
            far(g)

    whole = win.at[:, REACH]
    for kind, (condition, _, _, target) in plan.items():
        @pl.when(condition)
        def _():
            pltpu.make_async_remote_copy(
                src_ref=whole, dst_ref=whole, send_sem=send_sem.at[kind],
                recv_sem=recv_sem.at[0, 0], device_id={"sp": target}, device_id_type=MESH,
            ).wait_send()


def leave(heads, win, hidden, q_rope, sums, tops, o_hbm, last_heads, sem):
    done = heads.shape[0]

    def put(source, i):
        at = pl.ds(i * HEAD_SIZE, HEAD_SIZE)
        pltpu.make_async_copy(source, o_hbm.at[:, at], sem).start()

    for i in range(done):
        put(heads.at[i], i)
    units = unit_rows(win.shape[3])
    attend_far(win, hidden, q_rope, sums, tops, units, win.shape[0] - 1, last_heads, 0)
    for i in range(last_heads.shape[0]):
        put(last_heads.at[i], done + i)
    pltpu.make_async_copy(o_hbm, o_hbm, sem).wait()


def solution(mesh):
    count = mesh.shape["sp"]

    def body(query_proj, key_projection, value_projection, query_gain, key_norm_gain, positions, doc_start):
        rows = query_proj.shape[0]
        groups = key_projection.shape[1] // HEAD_SIZE
        copies = query_proj.shape[1] // key_projection.shape[1]
        assert rows * REACH >= DOC_MAX and count % 4 == 0
        assert rows == HEAD_SIZE and groups >= 6 and copies % Q_TILE == 0
        half_dim = HEAD_SIZE // 2
        inv_freq = ROPE_BASE ** (-(np.arange(half_dim) * 2.0 / HEAD_SIZE))
        freq = jnp.asarray(np.concatenate([inv_freq, inv_freq])[None, :], jnp.float32)
        blocks = REACH + 1
        tiles, tile_rows = copies // Q_TILE, Q_TILE * rows
        held = [
            jax.ShapeDtypeStruct(((groups - 1) * copies, rows, HEAD_SIZE), jnp.bfloat16),
            jax.ShapeDtypeStruct((groups, blocks, 2, rows, HEAD_SIZE), jnp.bfloat16),
            jax.ShapeDtypeStruct((blocks, rows, rows), jnp.bfloat16),
            jax.ShapeDtypeStruct((groups, copies * rows, HEAD_SIZE), jnp.bfloat16),
            jax.ShapeDtypeStruct((groups, tiles, tile_rows, 2 * HEAD_SIZE), jnp.float32),
            jax.ShapeDtypeStruct((groups, tiles, tile_rows, HEAD_SIZE), jnp.float32),
        ]
        state = pl.pallas_call(
            functools.partial(kernel, count, groups, copies, rows),
            out_shape=held,
            in_specs=[pl.BlockSpec(memory_space=pl.ANY)] * 8,
            out_specs=[pl.BlockSpec(memory_space=pltpu.VMEM)] * len(held),
            scratch_shapes=[
                pltpu.VMEM((groups * copies, rows, HEAD_SIZE), jnp.bfloat16),
                pltpu.VMEM(key_projection.shape, jnp.bfloat16),
                pltpu.VMEM((1, HEAD_SIZE), jnp.float32),
                pltpu.VMEM((1, HEAD_SIZE), jnp.float32),
                pltpu.VMEM((1, HEAD_SIZE), jnp.float32),
                pltpu.VMEM((1, rows), jnp.int32),
                pltpu.VMEM((1, rows), jnp.int32),
                pltpu.SemaphoreType.DMA((2,)),
                pltpu.SemaphoreType.DMA((6,)),
                pltpu.SemaphoreType.DMA((2,)),
                pltpu.SemaphoreType.DMA((10,)),
                pltpu.SemaphoreType.DMA((6, groups + 2)),
            ],
            compiler_params=pltpu.CompilerParams(
                collective_id=0, has_side_effects=True, vmem_limit_bytes=12 * 1024 * 1024
            ),
        )(
            *(pltpu.with_memory_space_constraint(array, pltpu.HBM) for array in (
                query_proj, key_projection, value_projection,
                query_gain[None, :], key_norm_gain[None, :], freq, positions[None, :], doc_start[None, :],
            ))
        )
        return pl.pallas_call(
            leave,
            out_shape=jax.ShapeDtypeStruct(query_proj.shape, jnp.bfloat16),
            in_specs=[pl.BlockSpec(memory_space=pltpu.VMEM)] * len(held),
            out_specs=pl.BlockSpec(memory_space=pl.ANY),
            scratch_shapes=[
                pltpu.VMEM((copies, rows, HEAD_SIZE), jnp.bfloat16), pltpu.SemaphoreType.DMA,
            ],
            compiler_params=pltpu.CompilerParams(vmem_limit_bytes=8 * 1024 * 1024),
        )(*state)

    tokens = P(("dp", "sp"), None)
    vector = P(("dp", "sp"))
    return jax.shard_map(
        body,
        mesh=mesh,
        in_specs=(tokens, tokens, tokens, P(), P(), vector, vector),
        out_specs=tokens,
        check_vma=False,
    )
```
